32 devices in a mesh: gx: 8 (over y, x, core), gy: 4 (over z).
Axes of the slice: x: 2, y: 2, z: 4, core: 2. Of those that a mesh axis runs over, the one named last changes fastest.
Arguments:
- theta: float32 [10, 128, 128, 128], P(None, 'gx', 'gy'), may hold values from -6 to 6
- phi_table: float32 [1024, 100], replicated, may hold values from -0.1 to 0.3
- dphi_table: float32 [1024, 100], replicated, may hold values from -0.5 to 1
Outputs:
- u_grids: float32 [10, 128, 128, 128], P(None, 'gx', 'gy')
- stress: float32 [3, 3], replicated
- energy: float32 [], replicated
The draws below stay inside these ranges and needn't reach their ends.
All inputs are finite; a program needn't handle non-finite values.
Results may differ from the reference program's by a relative error of at most 0.0003.
Values sent between devices are 32-bit elements; how exact they have to be, the bound alone decides.
No kernel may reach another device: no remote copies, remote signals or barrier semaphores. Data moves between devices by JAX's collectives and lax.ppermute only.
A program may use at most 128 MiB of HBM per device.

```python
import math
import jax
import jax.numpy as jnp
from jax import lax

NX = 128
NY = 128
NZ = 128
Q = 10
NK = 1024
QQ = 100


def steps_of(own_key, extent, shards, smallest, top_value):
    factor_of, own = 1.0, jax.random.fold_in(own_key, 6)
    for dim, parts in shards:
        heights = jnp.exp(jax.random.uniform(jax.random.fold_in(own, dim), (parts,), jnp.float32, smallest / len(shards), top_value / len(shards)))
        factor_of = factor_of * jnp.repeat(heights, extent[dim] // parts).reshape([-1 if axis == dim else 1 for axis in range(len(extent))])
    return factor_of


def normal_values(key, dims, spread, bound, pieces=(), kind=jnp.bfloat16):
    gain = steps_of(key, dims, pieces, -0.22, 0.18) if pieces else 1.0
    result = jax.random.normal(key, dims, jnp.float32) * spread * gain
    return jnp.minimum(jnp.maximum(result, -bound), bound).astype(kind)


def setup_inputs(seed: int = 0) -> dict:
    keys = jax.random.split(jax.random.key(seed), 4)
    return {
        "theta": normal_values(keys[0], (Q, NX, NY, NZ), 1.0, 6.0, ((1, 8), (2, 4)), jnp.float32),
        "phi_table": jnp.clip(jax.random.uniform(keys[1], (NK, QQ), jnp.float32, -0.1, 0.3), -0.1, 0.3),
        "dphi_table": jnp.clip(jax.random.uniform(keys[2], (NK, QQ), jnp.float32, -0.5, 1.0), -0.5, 1.0),
    }


HIGHEST = lax.Precision.HIGHEST

def wave_numbers(length):
    position = jnp.arange(length, dtype=jnp.int32)
    shifted = (position + length // 2) % length - length // 2
    return shifted.astype(jnp.float32) * (2.0 * math.pi / length)

def reference(theta, phi_table, dphi_table):
    spectrum = jnp.fft.fftn(theta, axes=(1, 2, 3))
    spec_real = jnp.real(spectrum)
    spec_imag = jnp.imag(spectrum)
    wave_x = wave_numbers(NX)
    wave_y = wave_numbers(NY)
    wave_z = wave_numbers(NZ)
    radial_scale = (NK - 1) / (math.pi * math.sqrt(3.0))
    grid_y = jnp.broadcast_to(wave_y[:, None], (NY, NZ))
    grid_z = jnp.broadcast_to(wave_z[None, :], (NY, NZ))

    def one_plane(plane_index):
        part_real = lax.dynamic_index_in_dim(spec_real, plane_index, 1, keepdims=False)
        part_imag = lax.dynamic_index_in_dim(spec_imag, plane_index, 1, keepdims=False)
        along_x = lax.dynamic_index_in_dim(wave_x, plane_index, 0, keepdims=False)
        radial = jnp.sqrt(along_x * along_x + grid_y * grid_y + grid_z * grid_z) * radial_scale
        lower_point = jnp.clip(jnp.floor(radial), 0.0, NK - 2.0)
        fraction = (radial - lower_point)[:, :, None]
        lower_index = lower_point.astype(jnp.int32)
        kernel = (1.0 - fraction) * phi_table[lower_index] + fraction * phi_table[lower_index + 1]
        kernel_slope = (1.0 - fraction) * dphi_table[lower_index] + fraction * dphi_table[lower_index + 1]
        kernel = kernel.reshape(NY, NZ, Q, Q)
        kernel_slope = kernel_slope.reshape(NY, NZ, Q, Q)
        u_real = jnp.einsum('yzqp,pyz->qyz', kernel, part_real, precision=HIGHEST)
        u_imag = jnp.einsum('yzqp,pyz->qyz', kernel, part_imag, precision=HIGHEST)
        grad_real = jnp.einsum('yzqp,pyz->qyz', kernel_slope, part_real, precision=HIGHEST)
        grad_imag = jnp.einsum('yzqp,pyz->qyz', kernel_slope, part_imag, precision=HIGHEST)
        weight = lax.optimization_barrier(jnp.sum(part_real * grad_real + part_imag * grad_imag, axis=0))
        moments = jnp.stack([jnp.sum(weight * along_x * along_x), jnp.sum(weight * grid_y * grid_y), jnp.sum(weight * grid_z * grid_z), jnp.sum(weight * along_x * grid_y), jnp.sum(weight * along_x * grid_z), jnp.sum(weight * grid_y * grid_z)])
        return (u_real, u_imag, moments)
    u_real, u_imag, moments = lax.map(one_plane, jnp.arange(NX, dtype=jnp.int32))
    u_spec = jnp.transpose(u_real + 1j * u_imag, (1, 0, 2, 3))
    u_grids = jnp.real(jnp.fft.ifftn(u_spec, axes=(1, 2, 3))).astype(jnp.float32)
    cell_total = NX * NY * NZ
    energy = jnp.sum(theta * u_grids) * (0.5 / cell_total)
    stress_terms = lax.optimization_barrier(jnp.sum(moments, axis=0)) * (-0.5 / (cell_total * cell_total))
    stress = jnp.stack([jnp.stack([stress_terms[0], stress_terms[3], stress_terms[4]]), jnp.stack([stress_terms[3], stress_terms[1], stress_terms[5]]), jnp.stack([stress_terms[4], stress_terms[5], stress_terms[2]])])
    return (u_grids, stress, energy)
```

```python
import functools
import math

import jax
import jax.numpy as jnp
import numpy as np
from jax import lax
from jax.experimental import pallas as pl
from jax.experimental.pallas import tpu as pltpu
from jax.sharding import PartitionSpec as P

HIGHEST = lax.Precision.HIGHEST
TWO_PI = 2.0 * math.pi


def signed_waves(position, length):
    shifted = (position + length // 2) % length - length // 2
    return shifted.astype(jnp.float32) * (TWO_PI / length)


def dft_table(row_freq, col_freq, length, direction):
    phase = row_freq[:, None] * col_freq[None, :] % length
    angle = phase.astype(jnp.float32) * (TWO_PI / length)
    return (jnp.cos(angle), direction * jnp.sin(angle))


def complex_turn(real_part, imag_part, cosine, sine, pattern):

    def product_of(first, second):
        return jnp.einsum(pattern, first, second, precision=HIGHEST)

    return (
        product_of(real_part, cosine) - product_of(imag_part, sine),
        product_of(real_part, sine) + product_of(imag_part, cosine),
    )


def contract_kernel(real_part, imag_part, wave_x, wave_y, wave_z, tables):
    q_count = real_part.shape[0]
    cell_count = real_part.shape[1]
    block_size = math.gcd(cell_count, 1024)
    table_points = tables.shape[0]
    pair_count = q_count * q_count
    radial_scale = (table_points - 1) / (math.pi * math.sqrt(3.0))

    def one_block(block_index, carry):
        u_real, u_imag, weight, energy_cells = carry
        offset = block_index * block_size
        part_real = lax.dynamic_slice_in_dim(real_part, offset, block_size, 1)
        part_imag = lax.dynamic_slice_in_dim(imag_part, offset, block_size, 1)
        along_x = lax.dynamic_slice_in_dim(wave_x, offset, block_size, 0)
        along_y = lax.dynamic_slice_in_dim(wave_y, offset, block_size, 0)
        along_z = lax.dynamic_slice_in_dim(wave_z, offset, block_size, 0)
        radial = jnp.sqrt(along_x * along_x + along_y * along_y + along_z * along_z) * radial_scale
        lower_point = jnp.clip(jnp.floor(radial), 0.0, table_points - 2.0)
        fraction = (radial - lower_point)[:, None]
        lower_index = lower_point.astype(jnp.int32)
        values = (1.0 - fraction) * tables[lower_index] + fraction * tables[lower_index + 1]
        kernel = values[:, :pair_count].reshape(block_size, q_count, q_count)
        kernel_slope = values[:, pair_count:].reshape(block_size, q_count, q_count)
        new_real = jnp.einsum("bqp,pb->qb", kernel, part_real, precision=HIGHEST)
        new_imag = jnp.einsum("bqp,pb->qb", kernel, part_imag, precision=HIGHEST)
        grad_real = jnp.einsum("bqp,pb->qb", kernel_slope, part_real, precision=HIGHEST)
        grad_imag = jnp.einsum("bqp,pb->qb", kernel_slope, part_imag, precision=HIGHEST)
        cell_weight = jnp.sum(part_real * grad_real + part_imag * grad_imag, axis=0)
        u_real = lax.dynamic_update_slice_in_dim(u_real, new_real, offset, 1)
        u_imag = lax.dynamic_update_slice_in_dim(u_imag, new_imag, offset, 1)
        weight = lax.dynamic_update_slice_in_dim(weight, cell_weight, offset, 0)
        cell_energy = jnp.sum(part_real * new_real + part_imag * new_imag, axis=0)
        energy_cells = lax.dynamic_update_slice_in_dim(energy_cells, cell_energy, offset, 0)
        return (u_real, u_imag, weight, energy_cells)

    start_carry = (
        jnp.zeros_like(real_part),
        jnp.zeros_like(imag_part),
        jnp.zeros((cell_count,), jnp.float32),
        jnp.zeros((cell_count,), jnp.float32),
    )
    return lax.fori_loop(0, cell_count // block_size, one_block, start_carry)


def moment_rows(weight, energy_cells, wave_x, wave_y, wave_z, item_count):
    stacked = (
        jnp.stack(
            [
                wave_x * wave_x,
                wave_y * wave_y,
                wave_z * wave_z,
                wave_x * wave_y,
                wave_x * wave_z,
                wave_y * wave_z,
            ]
        )
        * weight[None, :]
    )
    stacked = jnp.concatenate([energy_cells[None, :], stacked], axis=0)
    return jnp.sum(stacked.reshape(stacked.shape[0], item_count, -1), axis=2)


def general_shards(theta, phi_table, dphi_table):
    q_count, rows_x, rows_y, depth = theta.shape
    gx_size = lax.axis_size("gx")
    gy_size = lax.axis_size("gy")
    gx_index = lax.axis_index("gx")
    gy_index = lax.axis_index("gy")
    full_x = rows_x * gx_size
    full_y = rows_y * gy_size
    cell_total = full_x * full_y * depth
    tables = jnp.concatenate([phi_table, dphi_table], axis=1)
    z_points = jnp.arange(depth, dtype=jnp.int32)
    y_points = jnp.arange(full_y, dtype=jnp.int32)
    x_points = jnp.arange(full_x, dtype=jnp.int32)
    xc_fwd, xs_fwd = dft_table(x_points, x_points, full_x, -1.0)
    xc_back, xs_back = dft_table(x_points, x_points, full_x, 1.0)
    x_waves = signed_waves(x_points, full_x)
    zc_fwd, zs_fwd = dft_table(z_points, z_points, depth, -1.0)
    yc_fwd, ys_fwd = dft_table(y_points, y_points, full_y, -1.0)
    yc_back, ys_back = dft_table(y_points, y_points, full_y, 1.0)
    z_real = jnp.einsum("qxyn,nk->qkxy", theta, zc_fwd, precision=HIGHEST)
    z_imag = jnp.einsum("qxyn,nk->qkxy", theta, zs_fwd, precision=HIGHEST)
    s_real, s_imag = (
        lax.all_to_all(
            lax.all_to_all(z_real, "gx", split_axis=1, concat_axis=2, tiled=True),
            "gy",
            split_axis=1,
            concat_axis=3,
            tiled=True,
        ),
        lax.all_to_all(
            lax.all_to_all(z_imag, "gx", split_axis=1, concat_axis=2, tiled=True),
            "gy",
            split_axis=1,
            concat_axis=3,
            tiled=True,
        ),
    )
    slab_depth = depth // (gx_size * gy_size)
    z_first = gx_index * (depth // gx_size) + gy_index * slab_depth
    z_waves = signed_waves(z_first + jnp.arange(slab_depth, dtype=jnp.int32), depth)
    y_waves = signed_waves(y_points, full_y)
    a_real, a_imag = complex_turn(s_real, s_imag, xc_fwd, xs_fwd, "qzxy,xk->qzky")
    f_real, f_imag = complex_turn(a_real, a_imag, yc_fwd, ys_fwd, "qzxy,yk->qzxk")
    flat_cells = slab_depth * full_x * full_y
    grid_shape = (slab_depth, full_x, full_y)
    wave_z = jnp.broadcast_to(z_waves[:, None, None], grid_shape).reshape(flat_cells)
    wave_x = jnp.broadcast_to(x_waves[None, :, None], grid_shape).reshape(flat_cells)
    wave_y = jnp.broadcast_to(y_waves[None, None, :], grid_shape).reshape(flat_cells)
    u_real, u_imag, weight, energy_cells = contract_kernel(
        f_real.reshape(q_count, flat_cells),
        f_imag.reshape(q_count, flat_cells),
        wave_x,
        wave_y,
        wave_z,
        tables,
    )
    local_sums = moment_rows(weight, energy_cells, wave_x, wave_y, wave_z, 1)[:, 0]
    block_shape = (q_count, slab_depth, full_x, full_y)
    b_real, b_imag = complex_turn(
        u_real.reshape(block_shape), u_imag.reshape(block_shape), xc_back, xs_back, "qzky,kx->qzxy"
    )
    c_real, c_imag = complex_turn(b_real, b_imag, yc_back, ys_back, "qzxk,ky->qzxy")
    r_real, r_imag = (
        lax.all_to_all(
            lax.all_to_all(c_real, "gx", split_axis=2, concat_axis=1, tiled=True),
            "gy",
            split_axis=3,
            concat_axis=1,
            tiled=True,
        ),
        lax.all_to_all(
            lax.all_to_all(c_imag, "gx", split_axis=2, concat_axis=1, tiled=True),
            "gy",
            split_axis=3,
            concat_axis=1,
            tiled=True,
        ),
    )
    stride = gx_size * slab_depth
    positions = jnp.arange(depth, dtype=jnp.int32)
    z_order = (
        positions % stride // slab_depth * (depth // gx_size)
        + positions // stride * slab_depth
        + positions % slab_depth
    )
    zc_back, zs_back = dft_table(z_order, z_points, depth, 1.0)
    u_grids = (
        jnp.einsum("qzxy,zn->qxyn", r_real, zc_back, precision=HIGHEST)
        - jnp.einsum("qzxy,zn->qxyn", r_imag, zs_back, precision=HIGHEST)
    ) * (1.0 / cell_total)
    totals = lax.psum(local_sums, ("gx", "gy"))
    energy_scale = 0.5 / (cell_total * cell_total)
    energy = totals[0] * energy_scale
    stress_terms = totals[1:] * (-0.5 / (cell_total * cell_total))
    stress = stress_terms[np.array([0, 3, 4, 3, 1, 5, 4, 5, 2])].reshape(3, 3)
    return (u_grids, stress, energy)


LANES = 128
SUBLANES = 8
STATS = 7
AXES = ("gx", "gy")


def real_basis(length):
    half = length // 2
    points = np.arange(length)
    rows = []
    for index in range(length):
        number = index if index <= half else index - half
        angle = TWO_PI * (number * points % length) / length
        if index in (0, half):
            rows.append(np.cos(angle) / math.sqrt(length))
        elif index < half:
            rows.append(np.cos(angle) * math.sqrt(2.0 / length))
        else:
            rows.append(np.sin(angle) * math.sqrt(2.0 / length))
    return np.stack(rows)


def halves(table):
    high = np.asarray(table, dtype=jnp.bfloat16)
    low = np.asarray(table - high.astype(np.float64), dtype=jnp.bfloat16)
    return high, low


def split(value):
    high = value.astype(jnp.bfloat16)
    low = (value - high.astype(jnp.float32)).astype(jnp.bfloat16)
    return high, low


def product(left, right, contract_right=0):
    return lax.dot_general(
        left, right, (((1,), (contract_right,)), ((), ())), preferred_element_type=jnp.float32
    )


def z_forward_kernel(theta_ref, basis_ref, out_ref, *, q_count, groups, devices, rows):
    q = pl.program_id(0)
    high, low = split(theta_ref[0])
    spectrum = product(basis_ref[...], jnp.concatenate([high, low, high], axis=1), 1)
    for j in range(2):
        for g in range(groups):
            out_ref[pl.ds((g * 2 + j) * q_count + q, devices, stride=rows), :] = spectrum[
                j * devices : (j + 1) * devices, g * LANES : (g + 1) * LANES
            ]


def z_inverse_kernel(*refs, q_count, groups, devices, rows, slots):
    sent_refs, basis_ref, out_ref = refs[:slots], refs[slots], refs[slots + 1]
    q = pl.program_id(0)
    for g in range(groups):
        parts = []
        for sent_ref in sent_refs:
            for j in range(2):
                parts.append(
                    sent_ref[pl.ds((g * 2 + j) * q_count + q, devices, stride=rows), :]
                )
        high, low = split(jnp.transpose(jnp.concatenate(parts, axis=0)))
        out_ref[0, g * LANES : (g + 1) * LANES, :] = product(
            jnp.concatenate([high, low, high], axis=1), basis_ref[...]
        )


def fold(index, half):
    return jnp.where(index > half, index - half, index)


def table_kernel(planes_ref, bounds_ref, value_ref, step_ref, out_ref, *, half, pairs, group, scale, tiles, points):
    wave = math.pi / half
    row = lax.broadcasted_iota(jnp.int32, (SUBLANES, LANES), 0)
    wave_y = fold(lax.broadcasted_iota(jnp.int32, (SUBLANES, LANES), 1), half).astype(jnp.float32) * wave
    blocks = half // SUBLANES + 1

    def one_block(index, _):
        j = index // blocks
        block = index % blocks
        number = planes_ref[j]
        wave_z = number.astype(jnp.float32) * wave
        last = block == blocks - 1
        along_x = jnp.where(last, jnp.where(row == 0, half, row), row + block * SUBLANES)
        wave_x = along_x.astype(jnp.float32) * wave
        radial = jnp.sqrt(wave_x * wave_x + wave_y * wave_y + wave_z * wave_z) * scale
        lower = jnp.clip(jnp.floor(radial), 0.0, points - 2.0)
        fraction = radial - lower
        lower = lower.astype(jnp.int32)
        tile = lower // LANES
        lane = lower % LANES
        masks = [tile == t for t in range(tiles)]
        start = pl.multiple_of(block * SUBLANES, SUBLANES)

        def one_group(step, _):
            for i in range(group):
                pair = step * group + i
                value = jnp.zeros((SUBLANES, LANES), jnp.float32)
                slope = value
                for t in range(tiles):
                    def look(ref):
                        source = jnp.broadcast_to(ref[t, pl.ds(pair, 1), :], (SUBLANES, LANES))
                        return jnp.take_along_axis(source, lane, axis=1, mode="promise_in_bounds")
                    value = jnp.where(masks[t], look(value_ref), value)
                    slope = jnp.where(masks[t], look(step_ref), slope)
                out_ref[j, pair, pl.ds(start, SUBLANES), :] = value + fraction * slope
            return 0

        lax.fori_loop(0, pairs // group, one_group, 0)
        return 0

    lax.fori_loop(0, planes_ref[2] * blocks, one_block, 0)


def plane_kernel(
    planes_ref,
    waves_ref,
    sent_ref,
    y_ref,
    y_back_ref,
    x_ref,
    x_back_ref,
    table_hbm,
    out_ref,
    stats_ref,
    table_ref,
    y_wide_ref,
    y_back_wide_ref,
    rows_ref,
    spectrum_ref,
    u_ref,
    sem,
    *,
    q_count,
    gx_size,
    gy_size,
    rows,
    half,
):
    copy = pltpu.make_async_copy(table_hbm, table_ref, sem)
    copy.start()
    full = 2 * half
    local_y = full // gy_size
    spread = LANES // local_y
    planes = 2 * q_count
    strips = rows // planes
    high_x = gx_size * strips
    total_rows = gx_size * rows
    bf16 = jnp.bfloat16

    y_wide_ref[...] = jnp.zeros_like(y_wide_ref)
    for part in range(3):
        for s in range(gy_size):
            for k in range(spread):
                top = (part * gy_size + s) * LANES + k * local_y
                y_wide_ref[top : top + local_y, k * full : (k + 1) * full] = y_ref[
                    part, s * local_y : (s + 1) * local_y, :
                ]
    lane_part = lax.broadcasted_iota(jnp.int32, (full, gy_size * LANES), 1) // local_y % spread
    for part in range(3):
        for k in range(spread):
            top = (part * spread + k) * full
            y_back_wide_ref[top : top + full, :] = jnp.where(
                lane_part == k, y_back_ref[part].astype(jnp.float32), 0.0
            ).astype(bf16)

    for x in range(gx_size):
        highs, lows = [], []
        for s in range(gy_size):
            top = (x * gy_size + s) * rows
            high, low = split(sent_ref[top : top + rows, :])
            highs.append(high)
            lows.append(low)
        result = product(jnp.concatenate(highs + lows + highs, axis=1), y_wide_ref[...])
        for k in range(spread):
            top = k * total_rows + x * rows
            rows_ref[top : top + rows, :] = result[:, k * full : (k + 1) * full]

    for first in range(0, planes, 2):
        pair = []
        for plane in (first, first + 1):
            pair.append(
                jnp.concatenate(
                    [
                        rows_ref[pl.ds(k * total_rows + plane, high_x, stride=planes), :]
                        for k in range(spread)
                    ],
                    axis=0,
                )
            )
        high, low = split(jnp.concatenate(pair, axis=1))
        result = product(x_ref[...], jnp.concatenate([high, high, low], axis=0))
        for i in range(2):
            spectrum_ref[(first + i) * full : (first + i + 1) * full, :] = result[:, i * full : (i + 1) * full]

    copy.wait()
    wave = math.pi / half
    lane = lax.broadcasted_iota(jnp.int32, (SUBLANES, LANES), 1)
    row = lax.broadcasted_iota(jnp.int32, (SUBLANES, LANES), 0)
    wave_y = fold(lane, half).astype(jnp.float32) * wave
    signed_y = jnp.where(lane < half, wave_y, jnp.where(lane == half, 0.0, -wave_y))
    nyquist_y = jnp.where(lane == half, math.pi, 0.0)
    wave_z0, wave_z1, cross_z, nyquist_z = (waves_ref[i] for i in range(4))
    plane_index = (0, planes_ref[2] - 1)
    upper = {}
    for q in range(q_count):
        for p in range(q, q_count):
            upper[q, p] = upper[p, q] = q_count * q_count + len({k for k in upper if k[0] <= k[1]})

    def turn(value):
        return pltpu.roll(value, half, 1)

    def one_block(block, carry):
        energy, xx, yy, zz, xy, xz, yz = carry
        top = pl.multiple_of(block * SUBLANES, SUBLANES)
        tops = (top, pl.multiple_of(jnp.where(block == 0, half, top), SUBLANES))
        values = {}
        for j in range(2):
            for h in range(2):
                values[j, h] = [
                    spectrum_ref[pl.ds(pl.multiple_of((j * q_count + q) * full + h * half + top, SUBLANES), SUBLANES), :]
                    for q in range(q_count)
                ]
        zero = jnp.zeros((SUBLANES, LANES), jnp.float32)
        form = {key: zero for key in values}
        cross_xy, cross_xz, cross_yz = zero, zero, zero
        for q in range(q_count):
            bent = {}
            for key in values:
                j, h = key
                u = None
                for p in range(q_count):
                    term = table_ref[plane_index[j], q * q_count + p, pl.ds(tops[h], SUBLANES), :] * values[key][p]
                    u = term if u is None else u + term
                u_ref[pl.ds(pl.multiple_of((j * q_count + q) * full + h * half + top, SUBLANES), SUBLANES), :] = u
                energy = energy + u * values[key][q]
                v = None
                for p in range(q_count):
                    term = table_ref[plane_index[j], upper[q, p], pl.ds(tops[h], SUBLANES), :] * values[key][p]
                    v = term if v is None else v + term
                bent[key] = v
                form[key] = form[key] + v * values[key][q]
            cross_xy = cross_xy + bent[0, 0] * turn(values[0, 1][q]) + bent[1, 0] * turn(values[1, 1][q])
            cross_xz = cross_xz + bent[0, 0] * values[1, 1][q] - bent[1, 0] * values[0, 1][q]
            cross_yz = cross_yz + bent[0, 0] * turn(values[1, 0][q]) + bent[0, 1] * turn(values[1, 1][q])
        number = row + block * SUBLANES
        wave_c = number.astype(jnp.float32) * wave
        wave_s = jnp.where(number == 0, half, number).astype(jnp.float32) * wave
        nyquist_x = jnp.where(number == 0, math.pi, 0.0)
        xx = xx + (form[0, 0] + form[1, 0]) * (wave_c * wave_c) + (form[0, 1] + form[1, 1]) * (wave_s * wave_s)
        yy = yy + (form[0, 0] + form[1, 0] + form[0, 1] + form[1, 1]) * (wave_y * wave_y)
        zz = zz + (form[0, 0] + form[0, 1]) * (wave_z0 * wave_z0) + (form[1, 0] + form[1, 1]) * (wave_z1 * wave_z1)
        xy = xy - 2.0 * wave_c * signed_y * cross_xy + nyquist_x * nyquist_y * (form[0, 1] + form[1, 1])
        xz = xz - 2.0 * cross_z * wave_c * cross_xz + nyquist_z * nyquist_x * form[1, 1]
        yz = yz - 2.0 * cross_z * signed_y * cross_yz + nyquist_z * nyquist_y * (form[1, 0] + form[1, 1])
        return energy, xx, yy, zz, xy, xz, yz

    start = (jnp.zeros((SUBLANES, LANES), jnp.float32),) * STATS
    sums = lax.fori_loop(0, half // SUBLANES, one_block, start)
    stats_ref[...] = jnp.concatenate(
        [jnp.sum(part, axis=0, keepdims=True) for part in sums] + [jnp.zeros((1, LANES), jnp.float32)], axis=0
    )

    for first in range(0, planes, 2):
        high, low = split(
            jnp.concatenate(
                [u_ref[(first + i) * full : (first + i + 1) * full, :] for i in range(2)], axis=1
            )
        )
        result = product(x_back_ref[...], jnp.concatenate([high, high, low], axis=0))
        for i in range(2):
            for k in range(spread):
                rows_ref[pl.ds(k * total_rows + first + i, high_x, stride=planes), :] = result[
                    k * high_x : (k + 1) * high_x, i * full : (i + 1) * full
                ]

    for x in range(gx_size):
        strip = [rows_ref[k * total_rows + x * rows : k * total_rows + (x + 1) * rows, :] for k in range(spread)]
        high, low = split(jnp.concatenate(strip, axis=1))
        result = product(jnp.concatenate([high, low, high], axis=1), y_back_wide_ref[...])
        for s in range(gy_size):
            top = (x * gy_size + s) * rows
            out_ref[top : top + rows, :] = result[:, s * LANES : (s + 1) * LANES]


def table_rows(phi_table, dphi_table, q_count, padded):
    points = phi_table.shape[0]
    first = np.array([q * q_count + p for q in range(q_count) for p in range(q, q_count)])
    second = np.array([p * q_count + q for q in range(q_count) for p in range(q, q_count)])
    slopes = dphi_table.T
    slopes = 0.5 * (slopes[first] + slopes[second])
    table = jnp.concatenate([phi_table.T, slopes], axis=0)
    table = jnp.pad(table, ((0, padded - table.shape[0]), (0, 0)))
    steps = jnp.pad(table[:, 1:] - table[:, :-1], ((0, 0), (0, 1)))

    def tiled(values):
        return values.reshape(padded, points // LANES, LANES).transpose(1, 0, 2)

    return tiled(table), tiled(steps)


def butterfly(value, devices):
    step = 1
    while step < devices:
        value = value + lax.ppermute(value, AXES, [(i, i ^ step) for i in range(devices)])
        step *= 2
    return value


def swap(value, devices):
    parts = value.reshape(devices, -1, LANES)
    return lax.all_to_all(parts, AXES, split_axis=0, concat_axis=0, tiled=True).reshape(value.shape)


def real_shards(theta, phi_table, dphi_table):
    q_count, local_x, local_y, depth = theta.shape
    gx_size = lax.axis_size("gx")
    gy_size = lax.axis_size("gy")
    devices = gx_size * gy_size
    full = local_x * gx_size
    half = full // 2
    slots = depth // (2 * devices)
    groups = local_x * local_y // LANES
    spread = LANES // local_y
    rows = groups * 2 * q_count
    me = lax.axis_index("gx") * gy_size + lax.axis_index("gy")
    table_points = phi_table.shape[0]
    tiles = table_points // LANES
    upper_pairs = q_count * (q_count + 1) // 2
    group = 16
    padded = -(-(q_count * q_count + upper_pairs) // group) * group
    cell_total = full * full * depth
    vmem = pl.BlockSpec(memory_space=pltpu.VMEM)
    smem = pl.BlockSpec(memory_space=pltpu.SMEM)
    hbm = pl.BlockSpec(memory_space=pl.ANY)

    z_basis = real_basis(depth)
    basis = real_basis(full)

    def coefficient(slot, j):
        return slot if j == 0 else (depth // 2 + slot)

    order = [
        [coefficient(c * devices + d, j) for j in range(2) for d in range(devices)] for c in range(slots)
    ]
    flat_theta = theta.reshape(q_count, local_x * local_y, depth)
    sent = []
    for c in range(slots):
        high, low = halves(z_basis[order[c]])
        sent.append(
            pl.pallas_call(
                functools.partial(
                    z_forward_kernel, q_count=q_count, groups=groups, devices=devices, rows=rows
                ),
                grid=(q_count,),
                in_specs=[
                    pl.BlockSpec((1, local_x * local_y, depth), lambda q: (q, 0, 0)),
                    pl.BlockSpec((2 * devices, 3 * depth), lambda q: (0, 0)),
                ],
                out_specs=pl.BlockSpec((devices * rows, LANES), lambda q: (0, 0)),
                out_shape=jax.ShapeDtypeStruct((devices * rows, LANES), jnp.float32),
                name="z_forward",
            )(flat_theta, jnp.asarray(np.concatenate([high, high, low], axis=1)))
        )
    arrived = [swap(part, devices) for part in sent]

    value_table, step_table = table_rows(phi_table, dphi_table, q_count, padded)
    wave = math.pi / half
    scale = (table_points - 1) / (math.pi * math.sqrt(3.0))
    tables, settings = [], []
    blocks = half // SUBLANES + 1
    for c in range(slots):
        slot = c * devices + me
        special = slot == 0
        plane_numbers = jnp.stack(
            [slot, jnp.where(special, half, slot), jnp.where(special, 2, 1)]
        ).astype(jnp.int32)
        number = slot.astype(jnp.float32) * wave
        wave_values = jnp.stack(
            [
                number,
                jnp.where(special, math.pi, number),
                jnp.where(special, 0.0, number),
                jnp.where(special, math.pi, 0.0),
            ]
        )
        settings.append((plane_numbers, wave_values))
        tables.append(
            pl.pallas_call(
                functools.partial(
                    table_kernel,
                    half=half,
                    pairs=padded,
                    group=group,
                    scale=scale,
                    tiles=tiles,
                    points=table_points,
                ),
                in_specs=[smem, smem, vmem, vmem],
                out_specs=vmem,
                out_shape=jax.ShapeDtypeStruct((2, padded, blocks * SUBLANES, LANES), jnp.float32),
                name="kernel_table",
            )(plane_numbers, plane_numbers, value_table, step_table)
        )

    x_order = [
        (h // groups) * local_x + (h % groups) * spread + k for k in range(spread) for h in range(gx_size * groups)
    ]
    high, low = halves(basis[:, x_order])
    x_forward = jnp.asarray(np.concatenate([high, low, high], axis=1))
    x_back = jnp.asarray(np.concatenate([high.T, low.T, high.T], axis=1))
    high, low = halves(basis)
    y_forward = jnp.asarray(np.stack([high.T, high.T, low.T]))
    wide = [
        np.concatenate(
            [part[:, s * local_y : (s + 1) * local_y] for s in range(gy_size) for _ in range(spread)], axis=1
        )
        for part in (high, low)
    ]
    y_back = jnp.asarray(np.stack([wide[0], wide[0], wide[1]]))
    returned, stats = [], None
    for c in range(slots):
        back, part = pl.pallas_call(
            functools.partial(
                plane_kernel, q_count=q_count, gx_size=gx_size, gy_size=gy_size, rows=rows, half=half
            ),
            in_specs=[smem, smem, vmem, vmem, vmem, vmem, vmem, hbm],
            out_specs=(vmem, vmem),
            out_shape=(
                jax.ShapeDtypeStruct((devices * rows, LANES), jnp.float32),
                jax.ShapeDtypeStruct((SUBLANES, LANES), jnp.float32),
            ),
            scratch_shapes=[
                pltpu.VMEM((2, padded, blocks * SUBLANES, LANES), jnp.float32),
                pltpu.VMEM((3 * gy_size * LANES, spread * full), jnp.bfloat16),
                pltpu.VMEM((3 * spread * full, gy_size * LANES), jnp.bfloat16),
                pltpu.VMEM((spread * gx_size * rows, full), jnp.float32),
                pltpu.VMEM((2 * q_count * full, LANES), jnp.float32),
                pltpu.VMEM((2 * q_count * full, LANES), jnp.float32),
                pltpu.SemaphoreType.DMA,
            ],
            name="planes",
        )(*settings[c], arrived[c], y_forward, y_back, x_forward, x_back, tables[c])
        returned.append(swap(back, devices))
        stats = part if stats is None else stats + part

    high, low = halves(np.concatenate([z_basis[rows_of] for rows_of in order], axis=0))
    u_grids = pl.pallas_call(
        functools.partial(
            z_inverse_kernel, q_count=q_count, groups=groups, devices=devices, rows=rows, slots=slots
        ),
        grid=(q_count,),
        in_specs=[pl.BlockSpec((devices * rows, LANES), lambda q: (0, 0))] * slots
        + [pl.BlockSpec((3 * depth, depth), lambda q: (0, 0))],
        out_specs=pl.BlockSpec((1, local_x * local_y, depth), lambda q: (q, 0, 0)),
        out_shape=jax.ShapeDtypeStruct((q_count, local_x * local_y, depth), jnp.float32),
        name="z_inverse",
    )(*returned, jnp.asarray(np.concatenate([high, high, low], axis=0)))

    totals = jnp.sum(butterfly(stats, devices), axis=1)
    energy = totals[0] * (0.5 / cell_total)
    stress_terms = totals[1:STATS] * (-0.5 / cell_total)
    stress = stress_terms[np.array([0, 3, 4, 3, 1, 5, 4, 5, 2])].reshape(3, 3)
    return (u_grids.reshape(theta.shape), stress, energy)


def shards(theta, phi_table, dphi_table):
    q_count, local_x, local_y, depth = theta.shape
    gx_size = lax.axis_size("gx")
    gy_size = lax.axis_size("gy")
    devices = gx_size * gy_size
    fits = (
        local_x * gx_size == LANES
        and local_y * gy_size == LANES
        and depth == LANES
        and depth % (2 * devices) == 0
        and local_x * local_y % LANES == 0
        and phi_table.shape[0] % LANES == 0
        and devices & (devices - 1) == 0
        and (local_x * local_y // LANES) * q_count % 4 == 0
    )
    return (real_shards if fits else general_shards)(theta, phi_table, dphi_table)


def solution(mesh):
    return jax.shard_map(
        shards,
        mesh=mesh,
        in_specs=(P(None, "gx", "gy", None), P(), P()),
        out_specs=(P(None, "gx", "gy", None), P(), P()),
        check_vma=False,
    )
```

```python
import functools
import math

import jax
import jax.numpy as jnp
import numpy as np
from jax import lax
from jax.experimental import pallas as pl
from jax.experimental.pallas import tpu as pltpu
from jax.sharding import PartitionSpec as P


HIGHEST = lax.Precision.HIGHEST
TWO_PI = 2.0 * math.pi


def signed_waves(position, length):
    shifted = (position + length // 2) % length - length // 2
    return shifted.astype(jnp.float32) * (TWO_PI / length)


def dft_table(row_freq, col_freq, length, direction):
    phase = row_freq[:, None] * col_freq[None, :] % length
    angle = phase.astype(jnp.float32) * (TWO_PI / length)
    return (jnp.cos(angle), direction * jnp.sin(angle))


def complex_turn(real_part, imag_part, cosine, sine, pattern):

    def product_of(first, second):
        return jnp.einsum(pattern, first, second, precision=HIGHEST)

    return (
        product_of(real_part, cosine) - product_of(imag_part, sine),
        product_of(real_part, sine) + product_of(imag_part, cosine),
    )


def contract_kernel(real_part, imag_part, wave_x, wave_y, wave_z, tables):
    q_count = real_part.shape[0]
    cell_count = real_part.shape[1]
    block_size = math.gcd(cell_count, 1024)
    table_points = tables.shape[0]
    pair_count = q_count * q_count
    radial_scale = (table_points - 1) / (math.pi * math.sqrt(3.0))

    def one_block(block_index, carry):
        u_real, u_imag, weight, energy_cells = carry
        offset = block_index * block_size
        part_real = lax.dynamic_slice_in_dim(real_part, offset, block_size, 1)
        part_imag = lax.dynamic_slice_in_dim(imag_part, offset, block_size, 1)
        along_x = lax.dynamic_slice_in_dim(wave_x, offset, block_size, 0)
        along_y = lax.dynamic_slice_in_dim(wave_y, offset, block_size, 0)
        along_z = lax.dynamic_slice_in_dim(wave_z, offset, block_size, 0)
        radial = jnp.sqrt(along_x * along_x + along_y * along_y + along_z * along_z) * radial_scale
        lower_point = jnp.clip(jnp.floor(radial), 0.0, table_points - 2.0)
        fraction = (radial - lower_point)[:, None]
        lower_index = lower_point.astype(jnp.int32)
        values = (1.0 - fraction) * tables[lower_index] + fraction * tables[lower_index + 1]
        kernel = values[:, :pair_count].reshape(block_size, q_count, q_count)
        kernel_slope = values[:, pair_count:].reshape(block_size, q_count, q_count)
        new_real = jnp.einsum("bqp,pb->qb", kernel, part_real, precision=HIGHEST)
        new_imag = jnp.einsum("bqp,pb->qb", kernel, part_imag, precision=HIGHEST)
        grad_real = jnp.einsum("bqp,pb->qb", kernel_slope, part_real, precision=HIGHEST)
        grad_imag = jnp.einsum("bqp,pb->qb", kernel_slope, part_imag, precision=HIGHEST)
        cell_weight = jnp.sum(part_real * grad_real + part_imag * grad_imag, axis=0)
        u_real = lax.dynamic_update_slice_in_dim(u_real, new_real, offset, 1)
        u_imag = lax.dynamic_update_slice_in_dim(u_imag, new_imag, offset, 1)
        weight = lax.dynamic_update_slice_in_dim(weight, cell_weight, offset, 0)
        cell_energy = jnp.sum(part_real * new_real + part_imag * new_imag, axis=0)
        energy_cells = lax.dynamic_update_slice_in_dim(energy_cells, cell_energy, offset, 0)
        return (u_real, u_imag, weight, energy_cells)

    start_carry = (
        jnp.zeros_like(real_part),
        jnp.zeros_like(imag_part),
        jnp.zeros((cell_count,), jnp.float32),
        jnp.zeros((cell_count,), jnp.float32),
    )
    return lax.fori_loop(0, cell_count // block_size, one_block, start_carry)


def moment_rows(weight, energy_cells, wave_x, wave_y, wave_z, item_count):
    stacked = (
        jnp.stack(
            [
                wave_x * wave_x,
                wave_y * wave_y,
                wave_z * wave_z,
                wave_x * wave_y,
                wave_x * wave_z,
                wave_y * wave_z,
            ]
        )
        * weight[None, :]
    )
    stacked = jnp.concatenate([energy_cells[None, :], stacked], axis=0)
    return jnp.sum(stacked.reshape(stacked.shape[0], item_count, -1), axis=2)


def general_shards(theta, phi_table, dphi_table):
    q_count, rows_x, rows_y, depth = theta.shape
    gx_size = lax.axis_size("gx")
    gy_size = lax.axis_size("gy")
    gx_index = lax.axis_index("gx")
    gy_index = lax.axis_index("gy")
    full_x = rows_x * gx_size
    full_y = rows_y * gy_size
    cell_total = full_x * full_y * depth
    tables = jnp.concatenate([phi_table, dphi_table], axis=1)
    z_points = jnp.arange(depth, dtype=jnp.int32)
    y_points = jnp.arange(full_y, dtype=jnp.int32)
    x_points = jnp.arange(full_x, dtype=jnp.int32)
    xc_fwd, xs_fwd = dft_table(x_points, x_points, full_x, -1.0)
    xc_back, xs_back = dft_table(x_points, x_points, full_x, 1.0)
    x_waves = signed_waves(x_points, full_x)
    zc_fwd, zs_fwd = dft_table(z_points, z_points, depth, -1.0)
    yc_fwd, ys_fwd = dft_table(y_points, y_points, full_y, -1.0)
    yc_back, ys_back = dft_table(y_points, y_points, full_y, 1.0)
    z_real = jnp.einsum("qxyn,nk->qkxy", theta, zc_fwd, precision=HIGHEST)
    z_imag = jnp.einsum("qxyn,nk->qkxy", theta, zs_fwd, precision=HIGHEST)
    s_real, s_imag = (
        lax.all_to_all(
            lax.all_to_all(z_real, "gx", split_axis=1, concat_axis=2, tiled=True),
            "gy",
            split_axis=1,
            concat_axis=3,
            tiled=True,
        ),
        lax.all_to_all(
            lax.all_to_all(z_imag, "gx", split_axis=1, concat_axis=2, tiled=True),
            "gy",
            split_axis=1,
            concat_axis=3,
            tiled=True,
        ),
    )
    slab_depth = depth // (gx_size * gy_size)
    z_first = gx_index * (depth // gx_size) + gy_index * slab_depth
    z_waves = signed_waves(z_first + jnp.arange(slab_depth, dtype=jnp.int32), depth)
    y_waves = signed_waves(y_points, full_y)
    a_real, a_imag = complex_turn(s_real, s_imag, xc_fwd, xs_fwd, "qzxy,xk->qzky")
    f_real, f_imag = complex_turn(a_real, a_imag, yc_fwd, ys_fwd, "qzxy,yk->qzxk")
    flat_cells = slab_depth * full_x * full_y
    grid_shape = (slab_depth, full_x, full_y)
    wave_z = jnp.broadcast_to(z_waves[:, None, None], grid_shape).reshape(flat_cells)
    wave_x = jnp.broadcast_to(x_waves[None, :, None], grid_shape).reshape(flat_cells)
    wave_y = jnp.broadcast_to(y_waves[None, None, :], grid_shape).reshape(flat_cells)
    u_real, u_imag, weight, energy_cells = contract_kernel(
        f_real.reshape(q_count, flat_cells),
        f_imag.reshape(q_count, flat_cells),
        wave_x,
        wave_y,
        wave_z,
        tables,
    )
    local_sums = moment_rows(weight, energy_cells, wave_x, wave_y, wave_z, 1)[:, 0]
    block_shape = (q_count, slab_depth, full_x, full_y)
    b_real, b_imag = complex_turn(
        u_real.reshape(block_shape), u_imag.reshape(block_shape), xc_back, xs_back, "qzky,kx->qzxy"
    )
    c_real, c_imag = complex_turn(b_real, b_imag, yc_back, ys_back, "qzxk,ky->qzxy")
    r_real, r_imag = (
        lax.all_to_all(
            lax.all_to_all(c_real, "gx", split_axis=2, concat_axis=1, tiled=True),
            "gy",
            split_axis=3,
            concat_axis=1,
            tiled=True,
        ),
        lax.all_to_all(
            lax.all_to_all(c_imag, "gx", split_axis=2, concat_axis=1, tiled=True),
            "gy",
            split_axis=3,
            concat_axis=1,
            tiled=True,
        ),
    )
    stride = gx_size * slab_depth
    positions = jnp.arange(depth, dtype=jnp.int32)
    z_order = (
        positions % stride // slab_depth * (depth // gx_size)
        + positions // stride * slab_depth
        + positions % slab_depth
    )
    zc_back, zs_back = dft_table(z_order, z_points, depth, 1.0)
    u_grids = (
        jnp.einsum("qzxy,zn->qxyn", r_real, zc_back, precision=HIGHEST)
        - jnp.einsum("qzxy,zn->qxyn", r_imag, zs_back, precision=HIGHEST)
    ) * (1.0 / cell_total)
    totals = lax.psum(local_sums, ("gx", "gy"))
    energy_scale = 0.5 / (cell_total * cell_total)
    energy = totals[0] * energy_scale
    stress_terms = totals[1:] * (-0.5 / (cell_total * cell_total))
    stress = stress_terms[np.array([0, 3, 4, 3, 1, 5, 4, 5, 2])].reshape(3, 3)
    return (u_grids, stress, energy)


LANES = 128
SUBLANES = 8
STATS = 7
HALF_BITS = 16
MIDDLE = 1 << 15
AXES = ("gx", "gy")
WHOLE = 60 << 20


def real_basis(length):
    half = length // 2
    points = np.arange(length)
    rows = []
    for index in range(length):
        number = index if index <= half else index - half
        angle = TWO_PI * (number * points % length) / length
        if index in (0, half):
            rows.append(np.cos(angle) / math.sqrt(length))
        elif index < half:
            rows.append(np.cos(angle) * math.sqrt(2.0 / length))
        else:
            rows.append(np.sin(angle) * math.sqrt(2.0 / length))
    return np.stack(rows)


def halves(table):
    high = np.asarray(table, dtype=jnp.bfloat16)
    low = np.asarray(table - high.astype(np.float64), dtype=jnp.bfloat16)
    return high, low


def split(value):
    high = value.astype(jnp.bfloat16)
    low = (value - high.astype(jnp.float32)).astype(jnp.bfloat16)
    return high, low


def product(left, right, contract_right=0):
    return lax.dot_general(
        left, right, (((1,), (contract_right,)), ((), ())), preferred_element_type=jnp.float32
    )


def z_forward_kernel(theta_ref, basis_ref, out_ref, *, q_count, block, groups, devices, rows):
    basis = basis_ref[...]
    for k in range(block):
        high, low = split(theta_ref[k])
        spectrum = product(basis, jnp.concatenate([high, low, high], axis=1), 1)
        q = pl.program_id(0) * block + k
        for j in range(2):
            for g in range(groups):
                out_ref[pl.ds((g * 2 + j) * q_count + q, devices, stride=rows), :] = spectrum[
                    j * devices : (j + 1) * devices, g * LANES : (g + 1) * LANES
                ]


def pack_kernel(own_ref, near_ref, far_ref, *out_refs, rows):
    pieces = len(out_refs) // 2
    for k in range(pieces):
        block = slice(k * rows, (k + 1) * rows)
        out_refs[k][0:rows, :] = own_ref[block, :]
        out_refs[k][rows : 2 * rows, :] = near_ref[block, :]
        out_refs[k][2 * rows : 3 * rows, :] = far_ref[block, :]
        out_refs[pieces + k][...] = far_ref[(pieces + k) * rows : (pieces + k + 1) * rows, :]


def z_inverse_kernel(*refs, q_count, block, groups, devices, rows, last_rows, direct, gy_size, cell_total):
    gx_size = devices // gy_size
    pieces, refs = refs[: 2 * gx_size], refs[2 * gx_size :]
    direct_refs, refs = refs[:direct], refs[direct:]
    basis_ref, out_ref, stress_ref, energy_ref, first_ref = refs
    basis = basis_ref[...]

    @pl.when(pl.program_id(0) == 0)
    def _():
        my_x, my_y = lax.axis_index("gx"), lax.axis_index("gy")
        for k, piece in enumerate(pieces):
            for b, across in enumerate((0, 1, 2) if k < gx_size else (3,)):
                source = (my_x ^ (k % gx_size)) * gy_size + (my_y ^ across)
                first_ref[pl.ds(pl.multiple_of(source * rows, SUBLANES), rows), :] = piece[
                    b * rows : (b + 1) * rows, :
                ]
        last = direct_refs[-1]
        total = None
        for d in range(devices):
            part = last[(d + 1) * last_rows - SUBLANES : (d + 1) * last_rows, :]
            total = part if total is None else total + part
        terms = [jnp.sum(total[k : k + 1, :]) for k in range(STATS)]
        energy_ref[0, 0] = terms[0] * (0.5 / cell_total)
        for k, term in enumerate((0, 3, 4, 3, 1, 5, 4, 5, 2)):
            stress_ref[k // 3, k % 3] = terms[term + 1] * (-0.5 / cell_total)

    sources = [(first_ref, rows)] + [(ref, last_rows if ref is direct_refs[-1] else rows) for ref in direct_refs]
    for k in range(block):
        q = pl.program_id(0) * block + k
        for g in range(groups):
            parts = []
            for sent_ref, stride in sources:
                for j in range(2):
                    parts.append(sent_ref[pl.ds((g * 2 + j) * q_count + q, devices, stride=stride), :])
            high, low = split(jnp.transpose(jnp.concatenate(parts, axis=0)))
            out_ref[k, g * LANES : (g + 1) * LANES, :] = product(
                jnp.concatenate([high, low, high], axis=1), basis
            )


def fold(index, half):
    return jnp.where(index > half, index - half, index)


def device_number():
    return lax.axis_index("gx") * lax.axis_size("gy") + lax.axis_index("gy")


def fill_table(number, bounds_ref, scales_ref, words_ref, out_hbm, table_ref, found_ref, sem, *, half, pairs, scale, points):
    wave = math.pi / half
    row = lax.broadcasted_iota(jnp.int32, (SUBLANES, LANES), 0)
    wave_y = fold(lax.broadcasted_iota(jnp.int32, (SUBLANES, LANES), 1), half).astype(jnp.float32) * wave
    wave_z = number.astype(jnp.float32) * wave
    blocks = half // SUBLANES + 1

    def one_block(block, _):
        last = block == blocks - 1
        along_x = jnp.where(last, jnp.where(row == 0, half, row), row + block * SUBLANES)
        wave_x = along_x.astype(jnp.float32) * wave
        radial = jnp.sqrt(wave_x * wave_x + wave_y * wave_y + wave_z * wave_z) * scale
        lower = jnp.clip(jnp.floor(radial), 0.0, points - 2.0)
        fraction = radial - lower
        lower = lower.astype(jnp.int32)
        tile = lower // LANES
        lane = lower % LANES
        entry = (number * blocks + block) * 2

        def one_tile(t, _):
            mine = tile == t
            for pair in range(pairs):
                source = jnp.broadcast_to(words_ref[t, pair : pair + 1, :], (SUBLANES, LANES))
                found = jnp.take_along_axis(source, lane, axis=1, mode="promise_in_bounds")
                found_ref[pair] = jnp.where(mine, found, found_ref[pair])
            return 0

        lax.fori_loop(bounds_ref[entry], bounds_ref[entry + 1], one_tile, 0)
        for pair in range(pairs):
            word = found_ref[pair]
            below = (word >> HALF_BITS).astype(jnp.float32)
            above = (word & (2 * MIDDLE - 1)).astype(jnp.float32) - MIDDLE
            table_ref[block, pair] = (below + fraction * (above - below)) * scales_ref[pair]
        pltpu.make_async_copy(table_ref.at[block], out_hbm.at[block], sem).start()
        return 0

    lax.fori_loop(0, blocks, one_block, 0)
    pltpu.make_async_copy(table_ref, out_hbm, sem).wait()


def table_kernel(bounds_ref, scales_ref, words_ref, out_hbm, table_ref, found_ref, sem, *, base, **sizes):
    fill_table(base + device_number(), bounds_ref, scales_ref, words_ref, out_hbm, table_ref, found_ref, sem, **sizes)


def second_table_kernel(bounds_ref, scales_ref, words_ref, out_hbm, table_ref, found_ref, sem, *, base, **sizes):
    @pl.when(base + device_number() == 0)
    def _():
        fill_table(jnp.int32(sizes["half"]), bounds_ref, scales_ref, words_ref, out_hbm, table_ref, found_ref, sem, **sizes)


def tile_bounds(half, scale, points):
    blocks = half // SUBLANES + 1
    wave = math.pi / half
    bounds = []
    for number in range(half + 1):
        for block in range(blocks):
            low_x = 1 if block == blocks - 1 else block * SUBLANES
            high_x = half if block == blocks - 1 else block * SUBLANES + SUBLANES - 1
            low = math.sqrt(low_x**2 + number**2) * wave * scale - 0.1
            high = math.sqrt(high_x**2 + half**2 + number**2) * wave * scale + 0.1
            low, high = (int(min(max(math.floor(r), 0), points - 2)) // LANES for r in (low, high))
            bounds += [low, high + 1]
    return np.array(bounds, dtype=np.int32)


def mark_kernel(stats_ref, out_ref):
    out_ref[...] = stats_ref[...]


def plane_kernel(
    sent_ref,
    y_ref,
    y_back_ref,
    x_ref,
    x_back_ref,
    *rest,
    base,
    q_count,
    gx_size,
    gy_size,
    rows,
    out_rows,
    half,
    n_tables,
    hopped,
):
    before, rest = rest[: 1 - hopped], rest[1 - hopped :]
    tables, rest = rest[:n_tables], rest[n_tables:]
    my_x, my_y = lax.axis_index("gx"), lax.axis_index("gy")
    slot = base + device_number()
    special = slot == 0
    out_refs, rest = rest[: 1 + 2 * hopped], rest[1 + 2 * hopped :]
    stats_ref, y_wide_ref, y_back_wide_ref, rows_ref, spectrum_ref, u_ref, tables_ref, sem = rest
    first_copy = pltpu.make_async_copy(tables[0], tables_ref.at[0], sem.at[0])
    first_copy.start()
    if n_tables > 1:
        second_copy = pltpu.make_async_copy(tables[1], tables_ref.at[1], sem.at[1])

        @pl.when(special)
        def _():
            second_copy.start()

    full = 2 * half
    local_y = full // gy_size
    spread = LANES // local_y
    planes = 2 * q_count
    strips = rows // planes
    high_x = gx_size * strips
    total_rows = gx_size * rows
    bf16 = jnp.bfloat16

    y_wide_ref[...] = jnp.zeros_like(y_wide_ref)
    for part in range(3):
        for s in range(gy_size):
            for k in range(spread):
                top = (part * gy_size + s) * LANES + k * local_y
                y_wide_ref[top : top + local_y, k * full : (k + 1) * full] = y_ref[
                    part, s * local_y : (s + 1) * local_y, :
                ]
    lane_part = lax.broadcasted_iota(jnp.int32, (full, gy_size * LANES), 1) // local_y % spread
    for part in range(3):
        for k in range(spread):
            top = (part * spread + k) * full
            y_back_wide_ref[top : top + full, :] = jnp.where(
                lane_part == k, y_back_ref[part].astype(jnp.float32), 0.0
            ).astype(bf16)

    highs, lows = [], []
    for s in range(gy_size):
        tops = [(x * gy_size + s) * rows for x in range(gx_size)]
        high, low = split(jnp.concatenate([sent_ref[top : top + rows, :] for top in tops], axis=0))
        highs.append(high)
        lows.append(low)
    result = product(jnp.concatenate(highs + lows + highs, axis=1), y_wide_ref[...])
    for k in range(spread):
        rows_ref[k * total_rows : (k + 1) * total_rows, :] = result[:, k * full : (k + 1) * full]

    for first in range(0, planes, 2):
        pair = []
        for plane in (first, first + 1):
            pair.append(
                jnp.concatenate(
                    [
                        rows_ref[pl.ds(k * total_rows + plane, high_x, stride=planes), :]
                        for k in range(spread)
                    ],
                    axis=0,
                )
            )
        high, low = split(jnp.concatenate(pair, axis=1))
        result = product(x_ref[...], jnp.concatenate([high, high, low], axis=0))
        for i in range(2):
            spectrum_ref[(first + i) * full : (first + i + 1) * full, :] = result[:, i * full : (i + 1) * full]

    first_copy.wait()
    if n_tables > 1:

        @pl.when(special)
        def _():
            second_copy.wait()

    wave = math.pi / half
    lane = lax.broadcasted_iota(jnp.int32, (SUBLANES, LANES), 1)
    row = lax.broadcasted_iota(jnp.int32, (SUBLANES, LANES), 0)
    wave_y = fold(lane, half).astype(jnp.float32) * wave
    signed_y = jnp.where(lane < half, wave_y, jnp.where(lane == half, 0.0, -wave_y))
    nyquist_y = jnp.where(lane == half, math.pi, 0.0)
    wave_z0 = slot.astype(jnp.float32) * wave
    wave_z1 = jnp.where(special, math.pi, wave_z0)
    cross_z = wave_z0
    nyquist_z = jnp.where(special, math.pi, 0.0)
    table_of = (0, jnp.where(special, 1, 0) if n_tables > 1 else 0)
    upper = {}
    for q in range(q_count):
        for p in range(q, q_count):
            upper[q, p] = upper[p, q] = q_count * q_count + len({k for k in upper if k[0] <= k[1]})

    def turn(value):
        return pltpu.roll(value, half, 1)

    def one_block(block, carry):
        energy, xx, yy, zz, xy, xz, yz = carry
        top = pl.multiple_of(block * SUBLANES, SUBLANES)
        tops = (block, jnp.where(block == 0, half // SUBLANES, block))
        values = {}
        for j in range(2):
            for h in range(2):
                values[j, h] = [
                    spectrum_ref[pl.ds(pl.multiple_of((j * q_count + q) * full + h * half + top, SUBLANES), SUBLANES), :]
                    for q in range(q_count)
                ]
        zero = jnp.zeros((SUBLANES, LANES), jnp.float32)
        form = {key: zero for key in values}
        cross_xy, cross_xz, cross_yz = zero, zero, zero
        for q in range(q_count):
            bent = {}
            for key in values:
                j, h = key
                u = None
                for p in range(q_count):
                    term = tables_ref[table_of[j], tops[h], q * q_count + p] * values[key][p]
                    u = term if u is None else u + term
                u_ref[pl.ds(pl.multiple_of((j * q_count + q) * full + h * half + top, SUBLANES), SUBLANES), :] = u
                energy = energy + u * values[key][q]
                v = None
                for p in range(q_count):
                    term = tables_ref[table_of[j], tops[h], upper[q, p]] * values[key][p]
                    v = term if v is None else v + term
                bent[key] = v
                form[key] = form[key] + v * values[key][q]
            cross_xy = cross_xy + bent[0, 0] * turn(values[0, 1][q]) + bent[1, 0] * turn(values[1, 1][q])
            cross_xz = cross_xz + bent[0, 0] * values[1, 1][q] - bent[1, 0] * values[0, 1][q]
            cross_yz = cross_yz + bent[0, 0] * turn(values[1, 0][q]) + bent[0, 1] * turn(values[1, 1][q])
        number = row + block * SUBLANES
        wave_c = number.astype(jnp.float32) * wave
        wave_s = jnp.where(number == 0, half, number).astype(jnp.float32) * wave
        nyquist_x = jnp.where(number == 0, math.pi, 0.0)
        xx = xx + (form[0, 0] + form[1, 0]) * (wave_c * wave_c) + (form[0, 1] + form[1, 1]) * (wave_s * wave_s)
        yy = yy + (form[0, 0] + form[1, 0] + form[0, 1] + form[1, 1]) * (wave_y * wave_y)
        zz = zz + (form[0, 0] + form[0, 1]) * (wave_z0 * wave_z0) + (form[1, 0] + form[1, 1]) * (wave_z1 * wave_z1)
        xy = xy - 2.0 * wave_c * signed_y * cross_xy + nyquist_x * nyquist_y * (form[0, 1] + form[1, 1])
        xz = xz - 2.0 * cross_z * wave_c * cross_xz + nyquist_z * nyquist_x * form[1, 1]
        yz = yz - 2.0 * cross_z * signed_y * cross_yz + nyquist_z * nyquist_y * (form[1, 0] + form[1, 1])
        return energy, xx, yy, zz, xy, xz, yz

    start = (jnp.zeros((SUBLANES, LANES), jnp.float32),) * STATS
    sums = lax.fori_loop(0, half // SUBLANES, one_block, start)
    sums = jnp.concatenate(
        [jnp.sum(part, axis=0, keepdims=True) for part in sums] + [jnp.zeros((1, LANES), jnp.float32)], axis=0
    )

    stats_ref[...] = before[0][...] + sums if before else sums

    for first in range(0, planes, 2):
        high, low = split(
            jnp.concatenate(
                [u_ref[(first + i) * full : (first + i + 1) * full, :] for i in range(2)], axis=1
            )
        )
        result = product(x_back_ref[...], jnp.concatenate([high, high, low], axis=0))
        for i in range(2):
            for k in range(spread):
                rows_ref[pl.ds(k * total_rows + first + i, high_x, stride=planes), :] = result[
                    k * high_x : (k + 1) * high_x, i * full : (i + 1) * full
                ]

    strips_of = [split(rows_ref[k * total_rows : (k + 1) * total_rows, :]) for k in range(spread)]
    highs = [part[0] for part in strips_of]
    lows = [part[1] for part in strips_of]
    result = product(jnp.concatenate(highs + lows + highs, axis=1), y_back_wide_ref[...])
    half_y = gy_size // 2
    for x in range(gx_size):
        for s in range(gy_size):
            value = result[x * rows : (x + 1) * rows, s * LANES : (s + 1) * LANES]
            if hopped:
                across = my_y ^ s
                near_top = pl.multiple_of((my_x ^ x) * rows, SUBLANES)
                far_top = pl.multiple_of(((across % half_y) * gx_size + (my_x ^ x)) * rows, SUBLANES)

                @pl.when(across == 0)
                def _(value=value, top=near_top):
                    out_refs[0][pl.ds(top, rows), :] = value

                @pl.when(across == 1)
                def _(value=value, top=near_top):
                    out_refs[1][pl.ds(top, rows), :] = value

                @pl.when(across >= half_y)
                def _(value=value, top=far_top):
                    out_refs[2][pl.ds(top, rows), :] = value

            else:
                top = (x * gy_size + s) * out_rows
                out_refs[0][top : top + rows, :] = value
                if out_rows > rows:
                    out_refs[0][top + rows : top + out_rows, :] = stats_ref[...]


def table_rows(phi_table, dphi_table, q_count, padded):
    points = phi_table.shape[0]
    first = np.array([q * q_count + p for q in range(q_count) for p in range(q, q_count)])
    second = np.array([p * q_count + q for q in range(q_count) for p in range(q, q_count)])
    slopes = dphi_table.T
    slopes = 0.5 * (slopes[first] + slopes[second])
    table = jnp.concatenate([phi_table.T, slopes], axis=0)
    top = jnp.max(jnp.abs(table), axis=1)
    scales = jnp.where(top > 0.0, top, 1.0) / (MIDDLE - 1)
    steps = jnp.round(table / scales[:, None]).astype(jnp.int32)
    following = jnp.concatenate([steps[:, 1:], steps[:, -1:]], axis=1)
    words = steps * (2 * MIDDLE) + (following + MIDDLE)
    words = jnp.pad(words, ((0, padded - words.shape[0]), (0, 0)))
    return words.reshape(padded, points // LANES, LANES).transpose(1, 0, 2), scales


def swap(value, devices):
    parts = value.reshape(devices, -1, LANES)
    return lax.all_to_all(parts, AXES, split_axis=0, concat_axis=0, tiled=True).reshape(value.shape)


def real_shards(theta, phi_table, dphi_table):
    q_count, local_x, local_y, depth = theta.shape
    gx_size = lax.axis_size("gx")
    gy_size = lax.axis_size("gy")
    devices = gx_size * gy_size
    full = local_x * gx_size
    half = full // 2
    slots = depth // (2 * devices)
    groups = local_x * local_y // LANES
    spread = LANES // local_y
    rows = groups * 2 * q_count
    table_points = phi_table.shape[0]
    upper_pairs = q_count * (q_count + 1) // 2
    pairs = q_count * q_count + upper_pairs
    padded = -(-pairs // SUBLANES) * SUBLANES
    cell_total = full * full * depth
    vmem = pl.BlockSpec(memory_space=pltpu.VMEM)
    smem = pl.BlockSpec(memory_space=pltpu.SMEM)
    hbm = pl.BlockSpec(memory_space=pl.ANY)

    z_basis = real_basis(depth)
    basis = real_basis(full)

    def coefficient(slot, j):
        return slot if j == 0 else (depth // 2 + slot)

    order = [
        [coefficient((slots - 1 - c) * devices + d, j) for j in range(2) for d in range(devices)]
        for c in range(slots)
    ]
    flat_theta = theta.reshape(q_count, local_x * local_y, depth)
    block = max(k for k in range(1, 6) if q_count % k == 0)
    arrived = []
    for c in range(slots):
        high, low = halves(z_basis[order[c]])
        sent = pl.pallas_call(
            functools.partial(
                z_forward_kernel,
                q_count=q_count,
                block=block,
                groups=groups,
                devices=devices,
                rows=rows,
            ),
            grid=(q_count // block,),
            in_specs=[
                pl.BlockSpec((block, local_x * local_y, depth), lambda q: (q, 0, 0)),
                pl.BlockSpec((2 * devices, 3 * depth), lambda q: (0, 0)),
            ],
            out_specs=pl.BlockSpec((devices * rows, LANES), lambda q: (0, 0)),
            out_shape=jax.ShapeDtypeStruct((devices * rows, LANES), jnp.float32),
            compiler_params=pltpu.CompilerParams(vmem_limit_bytes=WHOLE),
            name="z_forward",
        )(flat_theta, jnp.asarray(np.concatenate([high, high, low], axis=1)))
        arrived.append(swap(sent, devices))

    words, scales = table_rows(phi_table, dphi_table, q_count, padded)
    scale = (table_points - 1) / (math.pi * math.sqrt(3.0))
    bounds = jnp.asarray(tile_bounds(half, scale, table_points))
    tables = []
    blocks = half // SUBLANES + 1
    for c in range(slots):
        sizes = dict(base=(slots - 1 - c) * devices, half=half, pairs=pairs, scale=scale, points=table_points)
        table_shape = jax.ShapeDtypeStruct((blocks, pairs, SUBLANES, LANES), jnp.float32)
        params = pltpu.CompilerParams(vmem_limit_bytes=WHOLE)
        scratch = [
            pltpu.VMEM(table_shape.shape, jnp.float32),
            pltpu.VMEM((pairs, SUBLANES, LANES), jnp.int32),
            pltpu.SemaphoreType.DMA,
        ]
        found = [
            pl.pallas_call(
                functools.partial(table_kernel, **sizes),
                in_specs=[smem, smem, vmem],
                out_specs=hbm,
                out_shape=table_shape,
                scratch_shapes=scratch,
                compiler_params=params,
                name="kernel_table",
            )(bounds, scales, words)
        ]
        if c == slots - 1:
            found.append(
                pl.pallas_call(
                    functools.partial(second_table_kernel, **sizes),
                    in_specs=[smem, smem, vmem],
                    out_specs=hbm,
                    out_shape=table_shape,
                    scratch_shapes=scratch,
                    compiler_params=params,
                    name="second_table",
                )(bounds, scales, words)
            )
        tables.append(found)

    x_order = [
        (h // groups) * local_x + (h % groups) * spread + k for k in range(spread) for h in range(gx_size * groups)
    ]
    high, low = halves(basis[:, x_order])
    x_forward = jnp.asarray(np.concatenate([high, low, high], axis=1))
    x_back = jnp.asarray(np.concatenate([high.T, low.T, high.T], axis=1))
    high, low = halves(basis)
    y_forward = jnp.asarray(np.stack([high.T, high.T, low.T]))
    wide = [
        np.concatenate(
            [part[:, s * local_y : (s + 1) * local_y] for s in range(gy_size) for _ in range(spread)], axis=1
        )
        for part in (high, low)
    ]
    y_back = jnp.asarray(np.stack([wide[0], wide[0], wide[1]]))
    returned = []
    last_rows = rows + SUBLANES
    stats = ()
    for c in range(slots):
        hopped = c == 0
        out_rows = last_rows if c == slots - 1 else rows
        outs = [devices * out_rows]
        if hopped:
            outs = [gx_size * rows, gx_size * rows, 2 * gx_size * rows]
        *back, part = pl.pallas_call(
            functools.partial(
                plane_kernel,
                q_count=q_count,
                gx_size=gx_size,
                gy_size=gy_size,
                rows=rows,
                out_rows=out_rows,
                half=half,
                base=(slots - 1 - c) * devices,
                n_tables=len(tables[c]),
                hopped=hopped,
            ),
            in_specs=[vmem] * (5 + len(stats)) + [hbm] * len(tables[c]),
            out_specs=(vmem,) * (len(outs) + 1),
            out_shape=tuple(jax.ShapeDtypeStruct((count, LANES), jnp.float32) for count in outs)
            + (jax.ShapeDtypeStruct((SUBLANES, LANES), jnp.float32),),
            scratch_shapes=[
                pltpu.VMEM((3 * gy_size * LANES, spread * full), jnp.bfloat16),
                pltpu.VMEM((3 * spread * full, gy_size * LANES), jnp.bfloat16),
                pltpu.VMEM((spread * gx_size * rows, full), jnp.float32),
                pltpu.VMEM((2 * q_count * full, LANES), jnp.float32),
                pltpu.VMEM((2 * q_count * full, LANES), jnp.float32),
                pltpu.VMEM((len(tables[c]), blocks, pairs, SUBLANES, LANES), jnp.float32),
                pltpu.SemaphoreType.DMA((len(tables[c]),)),
            ],
            compiler_params=pltpu.CompilerParams(vmem_limit_bytes=WHOLE),
            name="planes",
        )(arrived[c], y_forward, y_back, x_forward, x_back, *stats, *tables[c])
        if hopped:
            def hop(value, step):
                return lax.ppermute(value, AXES, [(d, d ^ step) for d in range(devices)])

            far = hop(back[2], 2)
            near = hop(back[1], 1)
            gathered = pl.pallas_call(
                functools.partial(pack_kernel, rows=rows),
                in_specs=[vmem] * 3,
                out_specs=(vmem,) * (2 * gx_size),
                out_shape=(jax.ShapeDtypeStruct((3 * rows, LANES), jnp.float32),) * gx_size
                + (jax.ShapeDtypeStruct((rows, LANES), jnp.float32),) * gx_size,
                compiler_params=pltpu.CompilerParams(vmem_limit_bytes=WHOLE),
                name="pack",
            )(back[0], near, far)
            gathered = list(gathered)
            for k in [*range(gx_size, 2 * gx_size), *range(1, gx_size)]:
                gathered[k] = hop(gathered[k], k % gx_size * gy_size + k // gx_size)
            stats = (
                pl.pallas_call(
                    mark_kernel,
                    in_specs=[vmem],
                    out_specs=vmem,
                    out_shape=jax.ShapeDtypeStruct((SUBLANES, LANES), jnp.float32),
                    name="mark",
                )(part),
            )
        else:
            returned.append(swap(back[0], devices))

    high, low = halves(np.concatenate([z_basis[rows_of] for rows_of in order], axis=0))
    block = max(k for k in range(1, 6) if q_count % k == 0)
    u_grids, stress, energy = pl.pallas_call(
        functools.partial(
            z_inverse_kernel,
            q_count=q_count,
            block=block,
            groups=groups,
            devices=devices,
            rows=rows,
            last_rows=last_rows,
            direct=len(returned),
            gy_size=gy_size,
            cell_total=cell_total,
        ),
        grid=(q_count // block,),
        in_specs=[pl.BlockSpec(part.shape, lambda q: (0, 0)) for part in gathered + returned]
        + [pl.BlockSpec((3 * depth, depth), lambda q: (0, 0))],
        out_specs=(
            pl.BlockSpec((block, local_x * local_y, depth), lambda q: (q, 0, 0)),
            smem,
            smem,
        ),
        out_shape=(
            jax.ShapeDtypeStruct((q_count, local_x * local_y, depth), jnp.float32),
            jax.ShapeDtypeStruct((3, 3), jnp.float32),
            jax.ShapeDtypeStruct((1, 1), jnp.float32),
        ),
        scratch_shapes=[pltpu.VMEM((devices * rows, LANES), jnp.float32)],
        compiler_params=pltpu.CompilerParams(vmem_limit_bytes=WHOLE),
        name="z_inverse",
    )(*gathered, *returned, jnp.asarray(np.concatenate([high, high, low], axis=0)))
    return (u_grids.reshape(theta.shape), stress, energy.reshape(()))


def shards(theta, phi_table, dphi_table):
    q_count, local_x, local_y, depth = theta.shape
    gx_size = lax.axis_size("gx")
    gy_size = lax.axis_size("gy")
    devices = gx_size * gy_size
    fits = (
        local_x * gx_size == LANES
        and local_y * gy_size == LANES
        and depth == LANES
        and depth == 4 * devices
        and gy_size == 4
        and local_x * local_y % LANES == 0
        and phi_table.shape[0] % LANES == 0
        and devices & (devices - 1) == 0
        and (local_x * local_y // LANES) * q_count % 4 == 0
    )
    if not fits:
        return general_shards(theta, phi_table, dphi_table)
    return real_shards(theta, phi_table, dphi_table)


def solution(mesh):
    return jax.shard_map(
        shards,
        mesh=mesh,
        in_specs=(P(None, "gx", "gy", None), P(), P()),
        out_specs=(P(None, "gx", "gy", None), P(), P()),
        check_vma=False,
    )
```

```python
import functools
import math

import jax
import jax.numpy as jnp
import numpy as np
from jax import lax
from jax.experimental import pallas as pl
from jax.experimental.pallas import tpu as pltpu
from jax.sharding import PartitionSpec as P


HIGHEST = lax.Precision.HIGHEST
TWO_PI = 2.0 * math.pi


def signed_waves(position, length):
    shifted = (position + length // 2) % length - length // 2
    return shifted.astype(jnp.float32) * (TWO_PI / length)


def dft_table(row_freq, col_freq, length, direction):
    phase = row_freq[:, None] * col_freq[None, :] % length
    angle = phase.astype(jnp.float32) * (TWO_PI / length)
    return (jnp.cos(angle), direction * jnp.sin(angle))


def complex_turn(real_part, imag_part, cosine, sine, pattern):

    def product_of(first, second):
        return jnp.einsum(pattern, first, second, precision=HIGHEST)

    return (
        product_of(real_part, cosine) - product_of(imag_part, sine),
        product_of(real_part, sine) + product_of(imag_part, cosine),
    )


def contract_kernel(real_part, imag_part, wave_x, wave_y, wave_z, tables):
    q_count = real_part.shape[0]
    cell_count = real_part.shape[1]
    block_size = math.gcd(cell_count, 1024)
    table_points = tables.shape[0]
    pair_count = q_count * q_count
    radial_scale = (table_points - 1) / (math.pi * math.sqrt(3.0))

    def one_block(block_index, carry):
        u_real, u_imag, weight, energy_cells = carry
        offset = block_index * block_size
        part_real = lax.dynamic_slice_in_dim(real_part, offset, block_size, 1)
        part_imag = lax.dynamic_slice_in_dim(imag_part, offset, block_size, 1)
        along_x = lax.dynamic_slice_in_dim(wave_x, offset, block_size, 0)
        along_y = lax.dynamic_slice_in_dim(wave_y, offset, block_size, 0)
        along_z = lax.dynamic_slice_in_dim(wave_z, offset, block_size, 0)
        radial = jnp.sqrt(along_x * along_x + along_y * along_y + along_z * along_z) * radial_scale
        lower_point = jnp.clip(jnp.floor(radial), 0.0, table_points - 2.0)
        fraction = (radial - lower_point)[:, None]
        lower_index = lower_point.astype(jnp.int32)
        values = (1.0 - fraction) * tables[lower_index] + fraction * tables[lower_index + 1]
        kernel = values[:, :pair_count].reshape(block_size, q_count, q_count)
        kernel_slope = values[:, pair_count:].reshape(block_size, q_count, q_count)
        new_real = jnp.einsum("bqp,pb->qb", kernel, part_real, precision=HIGHEST)
        new_imag = jnp.einsum("bqp,pb->qb", kernel, part_imag, precision=HIGHEST)
        grad_real = jnp.einsum("bqp,pb->qb", kernel_slope, part_real, precision=HIGHEST)
        grad_imag = jnp.einsum("bqp,pb->qb", kernel_slope, part_imag, precision=HIGHEST)
        cell_weight = jnp.sum(part_real * grad_real + part_imag * grad_imag, axis=0)
        u_real = lax.dynamic_update_slice_in_dim(u_real, new_real, offset, 1)
        u_imag = lax.dynamic_update_slice_in_dim(u_imag, new_imag, offset, 1)
        weight = lax.dynamic_update_slice_in_dim(weight, cell_weight, offset, 0)
        cell_energy = jnp.sum(part_real * new_real + part_imag * new_imag, axis=0)
        energy_cells = lax.dynamic_update_slice_in_dim(energy_cells, cell_energy, offset, 0)
        return (u_real, u_imag, weight, energy_cells)

    start_carry = (
        jnp.zeros_like(real_part),
        jnp.zeros_like(imag_part),
        jnp.zeros((cell_count,), jnp.float32),
        jnp.zeros((cell_count,), jnp.float32),
    )
    return lax.fori_loop(0, cell_count // block_size, one_block, start_carry)


def moment_rows(weight, energy_cells, wave_x, wave_y, wave_z, item_count):
    stacked = (
        jnp.stack(
            [
                wave_x * wave_x,
                wave_y * wave_y,
                wave_z * wave_z,
                wave_x * wave_y,
                wave_x * wave_z,
                wave_y * wave_z,
            ]
        )
        * weight[None, :]
    )
    stacked = jnp.concatenate([energy_cells[None, :], stacked], axis=0)
    return jnp.sum(stacked.reshape(stacked.shape[0], item_count, -1), axis=2)


def general_shards(theta, phi_table, dphi_table):
    q_count, rows_x, rows_y, depth = theta.shape
    gx_size = lax.axis_size("gx")
    gy_size = lax.axis_size("gy")
    gx_index = lax.axis_index("gx")
    gy_index = lax.axis_index("gy")
    full_x = rows_x * gx_size
    full_y = rows_y * gy_size
    cell_total = full_x * full_y * depth
    tables = jnp.concatenate([phi_table, dphi_table], axis=1)
    z_points = jnp.arange(depth, dtype=jnp.int32)
    y_points = jnp.arange(full_y, dtype=jnp.int32)
    x_points = jnp.arange(full_x, dtype=jnp.int32)
    xc_fwd, xs_fwd = dft_table(x_points, x_points, full_x, -1.0)
    xc_back, xs_back = dft_table(x_points, x_points, full_x, 1.0)
    x_waves = signed_waves(x_points, full_x)
    zc_fwd, zs_fwd = dft_table(z_points, z_points, depth, -1.0)
    yc_fwd, ys_fwd = dft_table(y_points, y_points, full_y, -1.0)
    yc_back, ys_back = dft_table(y_points, y_points, full_y, 1.0)
    z_real = jnp.einsum("qxyn,nk->qkxy", theta, zc_fwd, precision=HIGHEST)
    z_imag = jnp.einsum("qxyn,nk->qkxy", theta, zs_fwd, precision=HIGHEST)
    s_real, s_imag = (
        lax.all_to_all(
            lax.all_to_all(z_real, "gx", split_axis=1, concat_axis=2, tiled=True),
            "gy",
            split_axis=1,
            concat_axis=3,
            tiled=True,
        ),
        lax.all_to_all(
            lax.all_to_all(z_imag, "gx", split_axis=1, concat_axis=2, tiled=True),
            "gy",
            split_axis=1,
            concat_axis=3,
            tiled=True,
        ),
    )
    slab_depth = depth // (gx_size * gy_size)
    z_first = gx_index * (depth // gx_size) + gy_index * slab_depth
    z_waves = signed_waves(z_first + jnp.arange(slab_depth, dtype=jnp.int32), depth)
    y_waves = signed_waves(y_points, full_y)
    a_real, a_imag = complex_turn(s_real, s_imag, xc_fwd, xs_fwd, "qzxy,xk->qzky")
    f_real, f_imag = complex_turn(a_real, a_imag, yc_fwd, ys_fwd, "qzxy,yk->qzxk")
    flat_cells = slab_depth * full_x * full_y
    grid_shape = (slab_depth, full_x, full_y)
    wave_z = jnp.broadcast_to(z_waves[:, None, None], grid_shape).reshape(flat_cells)
    wave_x = jnp.broadcast_to(x_waves[None, :, None], grid_shape).reshape(flat_cells)
    wave_y = jnp.broadcast_to(y_waves[None, None, :], grid_shape).reshape(flat_cells)
    u_real, u_imag, weight, energy_cells = contract_kernel(
        f_real.reshape(q_count, flat_cells),
        f_imag.reshape(q_count, flat_cells),
        wave_x,
        wave_y,
        wave_z,
        tables,
    )
    local_sums = moment_rows(weight, energy_cells, wave_x, wave_y, wave_z, 1)[:, 0]
    block_shape = (q_count, slab_depth, full_x, full_y)
    b_real, b_imag = complex_turn(
        u_real.reshape(block_shape), u_imag.reshape(block_shape), xc_back, xs_back, "qzky,kx->qzxy"
    )
    c_real, c_imag = complex_turn(b_real, b_imag, yc_back, ys_back, "qzxk,ky->qzxy")
    r_real, r_imag = (
        lax.all_to_all(
            lax.all_to_all(c_real, "gx", split_axis=2, concat_axis=1, tiled=True),
            "gy",
            split_axis=3,
            concat_axis=1,
            tiled=True,
        ),
        lax.all_to_all(
            lax.all_to_all(c_imag, "gx", split_axis=2, concat_axis=1, tiled=True),
            "gy",
            split_axis=3,
            concat_axis=1,
            tiled=True,
        ),
    )
    stride = gx_size * slab_depth
    positions = jnp.arange(depth, dtype=jnp.int32)
    z_order = (
        positions % stride // slab_depth * (depth // gx_size)
        + positions // stride * slab_depth
        + positions % slab_depth
    )
    zc_back, zs_back = dft_table(z_order, z_points, depth, 1.0)
    u_grids = (
        jnp.einsum("qzxy,zn->qxyn", r_real, zc_back, precision=HIGHEST)
        - jnp.einsum("qzxy,zn->qxyn", r_imag, zs_back, precision=HIGHEST)
    ) * (1.0 / cell_total)
    totals = lax.psum(local_sums, ("gx", "gy"))
    energy_scale = 0.5 / (cell_total * cell_total)
    energy = totals[0] * energy_scale
    stress_terms = totals[1:] * (-0.5 / (cell_total * cell_total))
    stress = stress_terms[np.array([0, 3, 4, 3, 1, 5, 4, 5, 2])].reshape(3, 3)
    return (u_grids, stress, energy)


LANES = 128
SUBLANES = 8
STATS = 7
HALF_BITS = 16
MIDDLE = 1 << 15
AXES = ("gx", "gy")
WHOLE = 63 << 20
PART = 24 << 20


def real_basis(length):
    half = length // 2
    points = np.arange(length)
    rows = []
    for index in range(length):
        number = index if index <= half else index - half
        angle = TWO_PI * (number * points % length) / length
        if index in (0, half):
            rows.append(np.cos(angle) / math.sqrt(length))
        elif index < half:
            rows.append(np.cos(angle) * math.sqrt(2.0 / length))
        else:
            rows.append(np.sin(angle) * math.sqrt(2.0 / length))
    return np.stack(rows)


def halves(table):
    high = np.asarray(table, dtype=jnp.bfloat16)
    low = np.asarray(table - high.astype(np.float64), dtype=jnp.bfloat16)
    return high, low


def split(value):
    high = value.astype(jnp.bfloat16)
    low = (value - high.astype(jnp.float32)).astype(jnp.bfloat16)
    return high, low


def product(left, right, contract_right=0):
    return lax.dot_general(
        left, right, (((1,), (contract_right,)), ((), ())), preferred_element_type=jnp.float32
    )


def z_forward_kernel(theta_ref, basis_ref, out_ref, *, q_count, block, groups, devices, rows):
    basis = basis_ref[...]
    for k in range(block):
        high, low = split(theta_ref[k])
        spectrum = product(basis, jnp.concatenate([high, low, high], axis=1), 1)
        q = pl.program_id(0) * block + k
        for j in range(2):
            for g in range(groups):
                out_ref[pl.ds((g * 2 + j) * q_count + q, devices, stride=rows), :] = spectrum[
                    j * devices : (j + 1) * devices, g * LANES : (g + 1) * LANES
                ]


def pack_kernel(own_ref, near_ref, far_ref, stats_ref, far_stats_ref, *out_refs, rows):
    pieces = len(out_refs) // 2
    sums = stats_ref[...] + far_stats_ref[...]
    for k in range(pieces):
        block = slice(k * rows, (k + 1) * rows)
        out_refs[k][0:rows, :] = own_ref[block, :]
        out_refs[k][rows : 2 * rows, :] = near_ref[block, :]
        out_refs[k][2 * rows : 3 * rows, :] = far_ref[block, :]
        out_refs[k][3 * rows :, :] = sums
        out_refs[pieces + k][:rows, :] = far_ref[(pieces + k) * rows : (pieces + k + 1) * rows, :]
        out_refs[pieces + k][rows:, :] = sums


def z_inverse_kernel(*refs, q_count, block, groups, devices, rows, direct, gy_size, cell_total):
    gx_size = devices // gy_size
    pieces, refs = refs[: 2 * gx_size], refs[2 * gx_size :]
    direct_refs, refs = refs[:direct], refs[direct:]
    basis_ref, out_ref, stress_ref, energy_ref, first_ref, sums_ref = refs
    basis = basis_ref[...]

    @pl.when(pl.program_id(0) == 0)
    def _():
        my_x, my_y = lax.axis_index("gx"), lax.axis_index("gy")
        for k, piece in enumerate(pieces):
            for b, across in enumerate((0, 1, 2) if k < gx_size else (3,)):
                source = (my_x ^ (k % gx_size)) * gy_size + (my_y ^ across)
                first_ref[pl.ds(pl.multiple_of(source * rows, SUBLANES), rows), :] = piece[
                    b * rows : (b + 1) * rows, :
                ]
            pair = (my_x ^ (k % gx_size)) * 2 + (my_y ^ (k // gx_size)) % 2
            sums_ref[pl.ds(pl.multiple_of(pair * SUBLANES, SUBLANES), SUBLANES), :] = piece[-SUBLANES:, :]
        total = jnp.sum(sums_ref[...].reshape(devices // 2, SUBLANES, LANES), axis=0)
        terms = [jnp.sum(total[k : k + 1, :]) for k in range(STATS)]
        energy_ref[0, 0] = terms[0] * (0.5 / cell_total)
        for k, term in enumerate((0, 3, 4, 3, 1, 5, 4, 5, 2)):
            stress_ref[k // 3, k % 3] = terms[term + 1] * (-0.5 / cell_total)

    sources = [(ref, rows) for ref in (first_ref, *direct_refs)]
    for k in range(block):
        q = pl.program_id(0) * block + k
        for g in range(groups):
            parts = []
            for sent_ref, stride in sources:
                for j in range(2):
                    parts.append(sent_ref[pl.ds((g * 2 + j) * q_count + q, devices, stride=stride), :])
            high, low = split(jnp.transpose(jnp.concatenate(parts, axis=0)))
            out_ref[k, g * LANES : (g + 1) * LANES, :] = product(
                jnp.concatenate([high, low, high], axis=1), basis
            )


def fold(index, half):
    return jnp.where(index > half, index - half, index)


def device_number():
    return lax.axis_index("gx") * lax.axis_size("gy") + lax.axis_index("gy")


def fill_table(number, bounds_ref, scales_ref, words_ref, out_hbm, table_ref, found_ref, sem, *, half, pairs, scale, points):
    wave = math.pi / half
    row = lax.broadcasted_iota(jnp.int32, (SUBLANES, LANES), 0)
    wave_y = fold(lax.broadcasted_iota(jnp.int32, (SUBLANES, LANES), 1), half).astype(jnp.float32) * wave
    wave_z = number.astype(jnp.float32) * wave
    blocks = half // SUBLANES + 1

    def one_block(block, _):
        last = block == blocks - 1
        along_x = jnp.where(last, jnp.where(row == 0, half, row), row + block * SUBLANES)
        wave_x = along_x.astype(jnp.float32) * wave
        radial = jnp.sqrt(wave_x * wave_x + wave_y * wave_y + wave_z * wave_z) * scale
        lower = jnp.clip(jnp.floor(radial), 0.0, points - 2.0)
        fraction = radial - lower
        lower = lower.astype(jnp.int32)
        tile = lower // LANES
        lane = lower % LANES
        entry = (number * blocks + block) * 2

        def one_tile(t, _):
            mine = tile == t
            for pair in range(pairs):
                source = jnp.broadcast_to(words_ref[t, pair : pair + 1, :], (SUBLANES, LANES))
                found = jnp.take_along_axis(source, lane, axis=1, mode="promise_in_bounds")
                found_ref[pair] = jnp.where(mine, found, found_ref[pair])
            return 0

        lax.fori_loop(bounds_ref[entry], bounds_ref[entry + 1], one_tile, 0)
        for pair in range(pairs):
            word = found_ref[pair]
            below = (word >> HALF_BITS).astype(jnp.float32)
            above = (word & (2 * MIDDLE - 1)).astype(jnp.float32) - MIDDLE
            table_ref[block, pair] = (below + fraction * (above - below)) * scales_ref[pair]
        pltpu.make_async_copy(table_ref.at[block], out_hbm.at[block], sem).start()
        return 0

    lax.fori_loop(0, blocks, one_block, 0)
    pltpu.make_async_copy(table_ref, out_hbm, sem).wait()


def table_kernel(bounds_ref, scales_ref, words_ref, out_hbm, table_ref, found_ref, sem, *, base, **sizes):
    fill_table(base + device_number(), bounds_ref, scales_ref, words_ref, out_hbm, table_ref, found_ref, sem, **sizes)


def second_table_kernel(bounds_ref, scales_ref, words_ref, out_hbm, table_ref, found_ref, sem, *, base, **sizes):
    @pl.when(base + device_number() == 0)
    def _():
        fill_table(jnp.int32(sizes["half"]), bounds_ref, scales_ref, words_ref, out_hbm, table_ref, found_ref, sem, **sizes)


def tile_bounds(half, scale, points):
    blocks = half // SUBLANES + 1
    wave = math.pi / half
    bounds = []
    for number in range(half + 1):
        for block in range(blocks):
            low_x = 1 if block == blocks - 1 else block * SUBLANES
            high_x = half if block == blocks - 1 else block * SUBLANES + SUBLANES - 1
            low = math.sqrt(low_x**2 + number**2) * wave * scale - 0.1
            high = math.sqrt(high_x**2 + half**2 + number**2) * wave * scale + 0.1
            low, high = (int(min(max(math.floor(r), 0), points - 2)) // LANES for r in (low, high))
            bounds += [low, high + 1]
    return np.array(bounds, dtype=np.int32)


def mark_kernel(stats_ref, out_ref):
    out_ref[...] = stats_ref[...]


def plane_kernel(
    sent_ref,
    y_ref,
    y_back_ref,
    x_ref,
    x_back_ref,
    *rest,
    base,
    q_count,
    gx_size,
    gy_size,
    rows,
    half,
    n_tables,
    hopped,
):
    before, rest = rest[: 1 - hopped], rest[1 - hopped :]
    tables, rest = rest[:n_tables], rest[n_tables:]
    my_x, my_y = lax.axis_index("gx"), lax.axis_index("gy")
    slot = base + device_number()
    special = slot == 0
    out_refs, rest = rest[: 1 + 2 * hopped], rest[1 + 2 * hopped :]
    stats_ref, y_wide_ref, y_back_wide_ref, rows_ref, spectrum_ref, u_ref, tables_ref, sem = rest
    blocks = half // SUBLANES + 1
    table_order = [blocks - 1, *range(blocks - 1)]

    def table_copy(k, block):
        return pltpu.make_async_copy(tables[k].at[block], tables_ref.at[k, block], sem.at[k, block])

    for block in table_order:
        table_copy(0, block).start()
        if n_tables > 1:

            @pl.when(special)
            def _(block=block):
                table_copy(1, block).start()

    def wait_table(block):
        table_copy(0, block).wait()
        if n_tables > 1:

            @pl.when(special)
            def _():
                table_copy(1, block).wait()

    full = 2 * half
    local_y = full // gy_size
    spread = LANES // local_y
    planes = 2 * q_count
    strips = rows // planes
    high_x = gx_size * strips
    total_rows = gx_size * rows
    bf16 = jnp.bfloat16

    y_wide_ref[...] = jnp.zeros_like(y_wide_ref)
    for part in range(3):
        for s in range(gy_size):
            for k in range(spread):
                top = (part * gy_size + s) * LANES + k * local_y
                y_wide_ref[top : top + local_y, k * full : (k + 1) * full] = y_ref[
                    part, s * local_y : (s + 1) * local_y, :
                ]
    lane_part = lax.broadcasted_iota(jnp.int32, (full, gy_size * LANES), 1) // local_y % spread
    for part in range(3):
        for k in range(spread):
            top = (part * spread + k) * full
            y_back_wide_ref[top : top + full, :] = jnp.where(
                lane_part == k, y_back_ref[part].astype(jnp.float32), 0.0
            ).astype(bf16)

    highs, lows = [], []
    for s in range(gy_size):
        tops = [(x * gy_size + s) * rows for x in range(gx_size)]
        high, low = split(jnp.concatenate([sent_ref[top : top + rows, :] for top in tops], axis=0))
        highs.append(high)
        lows.append(low)
    result = product(jnp.concatenate(highs + lows + highs, axis=1), y_wide_ref[...])
    for k in range(spread):
        rows_ref[k * total_rows : (k + 1) * total_rows, :] = result[:, k * full : (k + 1) * full]

    for first in range(0, planes, 2):
        pair = []
        for plane in (first, first + 1):
            pair.append(
                jnp.concatenate(
                    [
                        rows_ref[pl.ds(k * total_rows + plane, high_x, stride=planes), :]
                        for k in range(spread)
                    ],
                    axis=0,
                )
            )
        high, low = split(jnp.concatenate(pair, axis=1))
        result = product(x_ref[...], jnp.concatenate([high, high, low], axis=0))
        for i in range(2):
            spectrum_ref[(first + i) * full : (first + i + 1) * full, :] = result[:, i * full : (i + 1) * full]

    wait_table(blocks - 1)
    wave = math.pi / half
    lane = lax.broadcasted_iota(jnp.int32, (SUBLANES, LANES), 1)
    row = lax.broadcasted_iota(jnp.int32, (SUBLANES, LANES), 0)
    wave_y = fold(lane, half).astype(jnp.float32) * wave
    signed_y = jnp.where(lane < half, wave_y, jnp.where(lane == half, 0.0, -wave_y))
    nyquist_y = jnp.where(lane == half, math.pi, 0.0)
    wave_z0 = slot.astype(jnp.float32) * wave
    wave_z1 = jnp.where(special, math.pi, wave_z0)
    cross_z = wave_z0
    nyquist_z = jnp.where(special, math.pi, 0.0)
    table_of = (0, jnp.where(special, 1, 0) if n_tables > 1 else 0)
    upper = {}
    for q in range(q_count):
        for p in range(q, q_count):
            upper[q, p] = upper[p, q] = q_count * q_count + len({k for k in upper if k[0] <= k[1]})

    def turn(value):
        return pltpu.roll(value, half, 1)

    def one_block(block, carry):
        energy, xx, yy, zz, xy, xz, yz = carry
        wait_table(block)
        top = pl.multiple_of(block * SUBLANES, SUBLANES)
        tops = (block, jnp.where(block == 0, half // SUBLANES, block))
        values = {}
        for j in range(2):
            for h in range(2):
                values[j, h] = [
                    spectrum_ref[pl.ds(pl.multiple_of((j * q_count + q) * full + h * half + top, SUBLANES), SUBLANES), :]
                    for q in range(q_count)
                ]
        zero = jnp.zeros((SUBLANES, LANES), jnp.float32)
        form = {key: zero for key in values}
        cross_xy, cross_xz, cross_yz = zero, zero, zero
        for q in range(q_count):
            bent = {}
            for key in values:
                j, h = key
                u = None
                for p in range(q_count):
                    term = tables_ref[table_of[j], tops[h], q * q_count + p] * values[key][p]
                    u = term if u is None else u + term
                u_ref[pl.ds(pl.multiple_of((j * q_count + q) * full + h * half + top, SUBLANES), SUBLANES), :] = u
                energy = energy + u * values[key][q]
                v = None
                for p in range(q_count):
                    term = tables_ref[table_of[j], tops[h], upper[q, p]] * values[key][p]
                    v = term if v is None else v + term
                bent[key] = v
                form[key] = form[key] + v * values[key][q]
            cross_xy = cross_xy + bent[0, 0] * turn(values[0, 1][q]) + bent[1, 0] * turn(values[1, 1][q])
            cross_xz = cross_xz + bent[0, 0] * values[1, 1][q] - bent[1, 0] * values[0, 1][q]
            cross_yz = cross_yz + bent[0, 0] * turn(values[1, 0][q]) + bent[0, 1] * turn(values[1, 1][q])
        number = row + block * SUBLANES
        wave_c = number.astype(jnp.float32) * wave
        wave_s = jnp.where(number == 0, half, number).astype(jnp.float32) * wave
        nyquist_x = jnp.where(number == 0, math.pi, 0.0)
        xx = xx + (form[0, 0] + form[1, 0]) * (wave_c * wave_c) + (form[0, 1] + form[1, 1]) * (wave_s * wave_s)
        yy = yy + (form[0, 0] + form[1, 0] + form[0, 1] + form[1, 1]) * (wave_y * wave_y)
        zz = zz + (form[0, 0] + form[0, 1]) * (wave_z0 * wave_z0) + (form[1, 0] + form[1, 1]) * (wave_z1 * wave_z1)
        xy = xy - 2.0 * wave_c * signed_y * cross_xy + nyquist_x * nyquist_y * (form[0, 1] + form[1, 1])
        xz = xz - 2.0 * cross_z * wave_c * cross_xz + nyquist_z * nyquist_x * form[1, 1]
        yz = yz - 2.0 * cross_z * signed_y * cross_yz + nyquist_z * nyquist_y * (form[1, 0] + form[1, 1])
        return energy, xx, yy, zz, xy, xz, yz

    start = (jnp.zeros((SUBLANES, LANES), jnp.float32),) * STATS
    sums = lax.fori_loop(0, half // SUBLANES, one_block, start)
    sums = jnp.concatenate(
        [jnp.sum(part, axis=0, keepdims=True) for part in sums] + [jnp.zeros((1, LANES), jnp.float32)], axis=0
    )

    stats_ref[...] = before[0][...] + sums if before else sums

    for first in range(0, planes, 2):
        high, low = split(
            jnp.concatenate(
                [u_ref[(first + i) * full : (first + i + 1) * full, :] for i in range(2)], axis=1
            )
        )
        result = product(x_back_ref[...], jnp.concatenate([high, high, low], axis=0))
        for i in range(2):
            for k in range(spread):
                rows_ref[pl.ds(k * total_rows + first + i, high_x, stride=planes), :] = result[
                    k * high_x : (k + 1) * high_x, i * full : (i + 1) * full
                ]

    strips_of = [split(rows_ref[k * total_rows : (k + 1) * total_rows, :]) for k in range(spread)]
    highs = [part[0] for part in strips_of]
    lows = [part[1] for part in strips_of]
    result = product(jnp.concatenate(highs + lows + highs, axis=1), y_back_wide_ref[...])
    half_y = gy_size // 2
    for x in range(gx_size):
        for s in range(gy_size):
            value = result[x * rows : (x + 1) * rows, s * LANES : (s + 1) * LANES]
            if hopped:
                across = my_y ^ s
                near_top = pl.multiple_of((my_x ^ x) * rows, SUBLANES)
                far_top = pl.multiple_of(((across % half_y) * gx_size + (my_x ^ x)) * rows, SUBLANES)

                @pl.when(across == 0)
                def _(value=value, top=near_top):
                    out_refs[0][pl.ds(top, rows), :] = value

                @pl.when(across == 1)
                def _(value=value, top=near_top):
                    out_refs[1][pl.ds(top, rows), :] = value

                @pl.when(across >= half_y)
                def _(value=value, top=far_top):
                    out_refs[2][pl.ds(top, rows), :] = value

            else:
                top = (x * gy_size + s) * rows
                out_refs[0][top : top + rows, :] = value


def table_rows(phi_table, dphi_table, q_count, padded):
    points = phi_table.shape[0]
    first = np.array([q * q_count + p for q in range(q_count) for p in range(q, q_count)])
    second = np.array([p * q_count + q for q in range(q_count) for p in range(q, q_count)])
    slopes = dphi_table.T
    slopes = 0.5 * (slopes[first] + slopes[second])
    table = jnp.concatenate([phi_table.T, slopes], axis=0)
    top = jnp.max(jnp.abs(table), axis=1)
    scales = jnp.where(top > 0.0, top, 1.0) / (MIDDLE - 1)
    steps = jnp.round(table / scales[:, None]).astype(jnp.int32)
    following = jnp.concatenate([steps[:, 1:], steps[:, -1:]], axis=1)
    words = steps * (2 * MIDDLE) + (following + MIDDLE)
    words = jnp.pad(words, ((0, padded - words.shape[0]), (0, 0)))
    return words.reshape(padded, points // LANES, LANES).transpose(1, 0, 2), scales


def swap(value, devices):
    parts = value.reshape(devices, -1, LANES)
    return lax.all_to_all(parts, AXES, split_axis=0, concat_axis=0, tiled=True).reshape(value.shape)


def real_shards(theta, phi_table, dphi_table):
    q_count, local_x, local_y, depth = theta.shape
    gx_size = lax.axis_size("gx")
    gy_size = lax.axis_size("gy")
    devices = gx_size * gy_size
    full = local_x * gx_size
    half = full // 2
    slots = depth // (2 * devices)
    groups = local_x * local_y // LANES
    spread = LANES // local_y
    rows = groups * 2 * q_count
    table_points = phi_table.shape[0]
    upper_pairs = q_count * (q_count + 1) // 2
    pairs = q_count * q_count + upper_pairs
    padded = -(-pairs // SUBLANES) * SUBLANES
    cell_total = full * full * depth
    vmem = pl.BlockSpec(memory_space=pltpu.VMEM)
    smem = pl.BlockSpec(memory_space=pltpu.SMEM)
    hbm = pl.BlockSpec(memory_space=pl.ANY)

    z_basis = real_basis(depth)
    basis = real_basis(full)

    def coefficient(slot, j):
        return slot if j == 0 else (depth // 2 + slot)

    order = [
        [coefficient((slots - 1 - c) * devices + d, j) for j in range(2) for d in range(devices)]
        for c in range(slots)
    ]
    flat_theta = theta.reshape(q_count, local_x * local_y, depth)
    block = max(k for k in range(1, 6) if q_count % k == 0)
    arrived = []
    for c in range(slots):
        high, low = halves(z_basis[order[c]])
        sent = pl.pallas_call(
            functools.partial(
                z_forward_kernel,
                q_count=q_count,
                block=block,
                groups=groups,
                devices=devices,
                rows=rows,
            ),
            grid=(q_count // block,),
            in_specs=[
                pl.BlockSpec((block, local_x * local_y, depth), lambda q: (q, 0, 0)),
                pl.BlockSpec((2 * devices, 3 * depth), lambda q: (0, 0)),
            ],
            out_specs=pl.BlockSpec((devices * rows, LANES), lambda q: (0, 0)),
            out_shape=jax.ShapeDtypeStruct((devices * rows, LANES), jnp.float32),
            compiler_params=pltpu.CompilerParams(vmem_limit_bytes=WHOLE),
            name="z_forward",
        )(flat_theta, jnp.asarray(np.concatenate([high, high, low], axis=1)))
        arrived.append(swap(sent, devices))

    words, scales = table_rows(phi_table, dphi_table, q_count, padded)
    scale = (table_points - 1) / (math.pi * math.sqrt(3.0))
    bounds = jnp.asarray(tile_bounds(half, scale, table_points))
    tables = []
    blocks = half // SUBLANES + 1
    for c in range(slots):
        sizes = dict(base=(slots - 1 - c) * devices, half=half, pairs=pairs, scale=scale, points=table_points)
        table_shape = jax.ShapeDtypeStruct((blocks, pairs, SUBLANES, LANES), jnp.float32)
        params = pltpu.CompilerParams(vmem_limit_bytes=WHOLE)
        scratch = [
            pltpu.VMEM(table_shape.shape, jnp.float32),
            pltpu.VMEM((pairs, SUBLANES, LANES), jnp.int32),
            pltpu.SemaphoreType.DMA,
        ]
        found = [
            pl.pallas_call(
                functools.partial(table_kernel, **sizes),
                in_specs=[smem, smem, vmem],
                out_specs=hbm,
                out_shape=table_shape,
                scratch_shapes=scratch,
                compiler_params=params,
                name="kernel_table",
            )(bounds, scales, words)
        ]
        if c == slots - 1:
            found.append(
                pl.pallas_call(
                    functools.partial(second_table_kernel, **sizes),
                    in_specs=[smem, smem, vmem],
                    out_specs=hbm,
                    out_shape=table_shape,
                    scratch_shapes=scratch,
                    compiler_params=params,
                    name="second_table",
                )(bounds, scales, words)
            )
        tables.append(found)

    x_order = [
        (h // groups) * local_x + (h % groups) * spread + k for k in range(spread) for h in range(gx_size * groups)
    ]
    high, low = halves(basis[:, x_order])
    x_forward = jnp.asarray(np.concatenate([high, low, high], axis=1))
    x_back = jnp.asarray(np.concatenate([high.T, low.T, high.T], axis=1))
    high, low = halves(basis)
    y_forward = jnp.asarray(np.stack([high.T, high.T, low.T]))
    wide = [
        np.concatenate(
            [part[:, s * local_y : (s + 1) * local_y] for s in range(gy_size) for _ in range(spread)], axis=1
        )
        for part in (high, low)
    ]
    y_back = jnp.asarray(np.stack([wide[0], wide[0], wide[1]]))

    def hop(value, step):
        return lax.ppermute(value, AXES, [(d, d ^ step) for d in range(devices)])

    returned = []
    stats = ()
    for c in range(slots):
        hopped = c == 0
        outs = [devices * rows]
        if hopped:
            outs = [gx_size * rows, gx_size * rows, 2 * gx_size * rows]
        *back, part = pl.pallas_call(
            functools.partial(
                plane_kernel,
                q_count=q_count,
                gx_size=gx_size,
                gy_size=gy_size,
                rows=rows,
                half=half,
                base=(slots - 1 - c) * devices,
                n_tables=len(tables[c]),
                hopped=hopped,
            ),
            in_specs=[vmem] * (5 + len(stats)) + [hbm] * len(tables[c]),
            out_specs=(vmem,) * (len(outs) + 1),
            out_shape=tuple(jax.ShapeDtypeStruct((count, LANES), jnp.float32) for count in outs)
            + (jax.ShapeDtypeStruct((SUBLANES, LANES), jnp.float32),),
            scratch_shapes=[
                pltpu.VMEM((3 * gy_size * LANES, spread * full), jnp.bfloat16),
                pltpu.VMEM((3 * spread * full, gy_size * LANES), jnp.bfloat16),
                pltpu.VMEM((spread * gx_size * rows, full), jnp.float32),
                pltpu.VMEM((2 * q_count * full, LANES), jnp.float32),
                pltpu.VMEM((2 * q_count * full, LANES), jnp.float32),
                pltpu.VMEM((len(tables[c]), blocks, pairs, SUBLANES, LANES), jnp.float32),
                pltpu.SemaphoreType.DMA((len(tables[c]), blocks)),
            ],
            compiler_params=pltpu.CompilerParams(vmem_limit_bytes=WHOLE),
            name="planes",
        )(arrived[c], y_forward, y_back, x_forward, x_back, *stats, *tables[c])
        if hopped:
            own = back[0]
            far = hop(back[2], 2)
            near = hop(back[1], 1)
            stats = (
                pl.pallas_call(
                    mark_kernel,
                    in_specs=[vmem],
                    out_specs=vmem,
                    out_shape=jax.ShapeDtypeStruct((SUBLANES, LANES), jnp.float32),
                    name="mark",
                )(part),
            )
        else:
            far_part = hop(part, 2)
            returned.append(swap(back[0], devices))

    gathered = pl.pallas_call(
        functools.partial(pack_kernel, rows=rows),
        in_specs=[vmem] * 5,
        out_specs=(vmem,) * (2 * gx_size),
        out_shape=(jax.ShapeDtypeStruct((3 * rows + SUBLANES, LANES), jnp.float32),) * gx_size
        + (jax.ShapeDtypeStruct((rows + SUBLANES, LANES), jnp.float32),) * gx_size,
        compiler_params=pltpu.CompilerParams(vmem_limit_bytes=PART),
        name="pack",
    )(own, near, far, part, far_part)
    gathered = list(gathered)
    for k in [*range(gx_size, 2 * gx_size), *range(1, gx_size)]:
        gathered[k] = hop(gathered[k], k % gx_size * gy_size + k // gx_size)

    high, low = halves(np.concatenate([z_basis[rows_of] for rows_of in order], axis=0))
    block = max(k for k in range(1, 6) if q_count % k == 0)
    u_grids, stress, energy = pl.pallas_call(
        functools.partial(
            z_inverse_kernel,
            q_count=q_count,
            block=block,
            groups=groups,
            devices=devices,
            rows=rows,
            direct=len(returned),
            gy_size=gy_size,
            cell_total=cell_total,
        ),
        grid=(q_count // block,),
        in_specs=[pl.BlockSpec(part.shape, lambda q: (0, 0)) for part in gathered + returned]
        + [pl.BlockSpec((3 * depth, depth), lambda q: (0, 0))],
        out_specs=(
            pl.BlockSpec((block, local_x * local_y, depth), lambda q: (q, 0, 0)),
            smem,
            smem,
        ),
        out_shape=(
            jax.ShapeDtypeStruct((q_count, local_x * local_y, depth), jnp.float32),
            jax.ShapeDtypeStruct((3, 3), jnp.float32),
            jax.ShapeDtypeStruct((1, 1), jnp.float32),
        ),
        scratch_shapes=[
            pltpu.VMEM((devices * rows, LANES), jnp.float32),
            pltpu.VMEM((devices // 2 * SUBLANES, LANES), jnp.float32),
        ],
        compiler_params=pltpu.CompilerParams(vmem_limit_bytes=PART),
        name="z_inverse",
    )(*gathered, *returned, jnp.asarray(np.concatenate([high, high, low], axis=0)))
    return (u_grids.reshape(theta.shape), stress, energy.reshape(()))


def shards(theta, phi_table, dphi_table):
    q_count, local_x, local_y, depth = theta.shape
    gx_size = lax.axis_size("gx")
    gy_size = lax.axis_size("gy")
    devices = gx_size * gy_size
    fits = (
        local_x * gx_size == LANES
        and local_y * gy_size == LANES
        and depth == LANES
        and depth == 4 * devices
        and gy_size == 4
        and local_x * local_y % LANES == 0
        and phi_table.shape[0] % LANES == 0
        and devices & (devices - 1) == 0
        and (local_x * local_y // LANES) * q_count % 4 == 0
    )
    if not fits:
        return general_shards(theta, phi_table, dphi_table)
    return real_shards(theta, phi_table, dphi_table)


def solution(mesh):
    return jax.shard_map(
        shards,
        mesh=mesh,
        in_specs=(P(None, "gx", "gy", None), P(), P()),
        out_specs=(P(None, "gx", "gy", None), P(), P()),
        check_vma=False,
    )
```
